32 devices in a mesh: band: 4 (over y, core), grid: 8 (over z, x).
Axes of the slice: x: 2, y: 2, z: 4, core: 2. Of those that a mesh axis runs over, the one named last changes fastest.
Arguments:
- orbitals: bfloat16 [64, 2, 16, 128, 128], P('band', None, 'grid'), may hold values from -1.5 to 1.5
- occupations: float32 [64], P('band'), may hold values from 0.2 to 2
Outputs:
- current: float32 [3, 16, 128, 128], P(None, 'grid', 'band')
The draws below stay inside these ranges and needn't reach their ends.
All inputs are finite; a program needn't handle non-finite values.
Results may differ from the reference program's by a relative error of at most 0.0003.
Values may be sent and summed in bfloat16 or wider, within the bound.
A program may use at most 64 MiB of HBM per device.

```python
import jax
import jax.numpy as jnp
from jax import lax

NX = 128
NY = 128
BANDS = 64
NZ = 16


def block_scale(key, extent, cuts, smallest, top_value):
    def one(axis_at, parts):
        steps = jax.random.uniform(jax.random.fold_in(jax.random.fold_in(key, 6), axis_at), (parts,), jnp.float32, smallest / len(cuts), top_value / len(cuts))
        return jnp.repeat(jnp.exp(steps), extent[axis_at] // parts).reshape((-1,) + (1,) * (len(extent) - axis_at - 1))

    level = one(*cuts[0])
    for cut in cuts[1:]:
        level = level * one(*cut)
    return level


def normal_values(key, shape, width, reach, pieces=(), held_as=jnp.bfloat16):
    entries = width * jax.random.normal(key, shape, jnp.float32)
    if pieces:
        entries = entries * block_scale(key, shape, pieces, -0.22, 0.18)
    return jnp.clip(entries, -reach, reach).astype(held_as)


def setup_inputs(seed: int = 0) -> dict:
    splits = jax.random.split(jax.random.key(seed), 3)
    return {
        "orbitals": normal_values(splits[0], (BANDS, 2, NZ, NX, NY), 0.25, 1.5, ((0, 4), (2, 8))),
        "occupations": jnp.clip(0.2 + 1.8 * jax.random.uniform(splits[1], (BANDS,), jnp.float32) ** block_scale(splits[1], (BANDS,), ((0, 4),), -0.2, 0.2), 0.2, 2.0),
    }


def derivative(values, direction):
    forward = jnp.roll(values, -1, direction) - jnp.roll(values, 1, direction)
    farther = jnp.roll(values, -2, direction) - jnp.roll(values, 2, direction)
    return (8.0 * forward - farther) / 12.0


def reference(orbitals, occupations):
    def advance(summed, item):
        orbital, weight = item
        real_part = orbital[0].astype(jnp.float32)
        imag_part = orbital[1].astype(jnp.float32)
        components = jnp.stack([real_part * derivative(imag_part, direction) - imag_part * derivative(real_part, direction) for direction in range(3)])
        return summed + weight * components, None

    initial = jnp.zeros((3, NZ, NX, NY), jnp.float32)
    summed, _ = lax.scan(advance, initial, (orbitals, occupations))
    return summed
```

```python
import functools

import jax
import jax.numpy as jnp
from jax import lax
from jax.experimental import pallas as pl
from jax.experimental.pallas import tpu as pltpu
from jax.sharding import PartitionSpec as P

TILE = 16
PAIRS = ((0, 1), (1, 2), (2, 3), (3, 4), (0, 2), (1, 3), (2, 4), (3, 5))


def stencil(n, flipped):
    row = lax.broadcasted_iota(jnp.int32, (n, n), 0)
    col = lax.broadcasted_iota(jnp.int32, (n, n), 1)
    d = col - row if flipped else row - col
    value = jnp.zeros((n, n), jnp.float32)
    for step, weight in ((1, 8.0), (-1, -8.0), (2, -1.0), (-2, 1.0)):
        hit = (d == step) | (d == step - n) | (d == step + n)
        value = jnp.where(hit, weight, value)
    return value.astype(jnp.bfloat16)


def kernel(
    nb, ng, occ_hbm, orb_ref, out_ref,
    occ_ref, own, mate, outer, inner, mx, my, plane_sum, plane_recv, zsend, inbox, final,
    occ_sem, own_sem, mate_send, mate_recv, outer_send, outer_recv, inner_send, inner_recv,
    plane_send_sem, plane_recv_sem, inbox_send, inbox_recv, final_send, final_recv, up_token, down_token,
):
    bands, _, depth, nx, ny = orb_ref.shape
    b = lax.axis_index("band")
    g = lax.axis_index("grid")
    odd = lax.rem(g, 2)
    turn = 1 - 2 * odd
    partner = g + turn
    ahead = lax.rem(g + 2 * turn + ng, ng)
    behind = lax.rem(g - 2 * turn + ng, ng)
    side = lax.rem(g - turn + ng, ng)
    layers = ng // 2
    layer = g // 2
    rows = nx // nb
    half = rows // 2
    chips = nb // 2
    chip = b // 2
    core = lax.rem(b, 2)

    load = pltpu.make_async_copy(orb_ref, own, own_sem)
    load.start()
    weights = pltpu.make_async_copy(occ_hbm, occ_ref, occ_sem)
    weights.start()

    barrier = pltpu.get_barrier_semaphore()
    peers = [lax.rem(b + k, nb) for k in range(1, nb)]
    pl.semaphore_signal(barrier, inc=1, device_id={"band": b, "grid": partner})
    for peer in peers:
        pl.semaphore_signal(barrier, inc=1, device_id={"band": peer, "grid": g})

    @pl.when(layer > 0)
    def _():
        pl.semaphore_signal(barrier, inc=1, device_id={"band": b, "grid": g - 2})

    @pl.when(layer < layers - 1)
    def _():
        pl.semaphore_signal(barrier, inc=1, device_id={"band": b, "grid": g + 2})

    ends = (layer == 0).astype(jnp.int32) + (layer == layers - 1).astype(jnp.int32)
    pl.semaphore_wait(barrier, nb + 2 - ends)

    def chunk_of(k):
        return 2 * lax.rem(chip + 1 + k % chips, chips) + k // chips

    def start_of(k, parity):
        return pl.multiple_of(chunk_of(k) * rows + parity * half, half)

    def to_mate(k):
        return pltpu.make_async_remote_copy(
            src_ref=orb_ref.at[:, :, :, pl.ds(start_of(k, 1 - odd), half), :],
            dst_ref=mate.at[k],
            send_sem=mate_send.at[k],
            recv_sem=mate_recv.at[k],
            device_id={"band": b, "grid": partner},
        )

    def to_outer(k):
        return pltpu.make_async_remote_copy(
            src_ref=orb_ref.at[:, :, :, pl.ds(start_of(k, odd), half), :],
            dst_ref=outer.at[k - chips],
            send_sem=outer_send.at[k - chips],
            recv_sem=outer_recv.at[k - chips],
            device_id={"band": b, "grid": behind},
        )

    def to_inner(k):
        return pltpu.make_async_remote_copy(
            src_ref=mate.at[k],
            dst_ref=inner.at[k],
            send_sem=inner_send.at[k],
            recv_sem=inner_recv.at[k],
            device_id={"band": b, "grid": ahead},
        )

    wraps = ((odd == 0) & (layer == 0)) | ((odd == 1) & (layer == layers - 1))
    for k in range(nb):
        to_mate(k).start()

    @pl.when(jnp.logical_not(wraps))
    def _():
        for k in range(chips, nb):
            to_outer(k).start()

    @pl.when(layer == 1)
    def _():
        pl.semaphore_signal(up_token, inc=1, device_id={"band": b, "grid": g + 2})

    @pl.when(layer == layers - 2)
    def _():
        pl.semaphore_signal(down_token, inc=1, device_id={"band": b, "grid": g - 2})

    @pl.when(layer >= 2)
    def _():
        pl.semaphore_wait(up_token, 1)

        @pl.when(layer < layers - 1)
        def _():
            pl.semaphore_signal(up_token, inc=1, device_id={"band": b, "grid": g + 2})

    @pl.when(layer <= layers - 3)
    def _():
        pl.semaphore_wait(down_token, 1)

        @pl.when(layer > 0)
        def _():
            pl.semaphore_signal(down_token, inc=1, device_id={"band": b, "grid": g - 2})

    @pl.when(wraps)
    def _():
        for k in range(chips, nb):
            to_outer(k).start()

    mx[...] = stencil(nx, True)
    my[...] = stencil(ny, False)
    plane_sum[...] = jnp.zeros_like(plane_sum)
    load.wait()
    weights.wait()

    def lateral(n, carry):
        w = occ_ref[n]
        for s in range(depth):
            re = own[n, 0, s]
            im = own[n, 1, s]
            tx = jnp.dot(mx[...], jnp.concatenate([re, im], 1), preferred_element_type=jnp.float32)
            ty = jnp.dot(jnp.concatenate([re, im], 0), my[...], preferred_element_type=jnp.float32)
            wre = re.astype(jnp.float32) * w
            wim = im.astype(jnp.float32) * w
            plane_sum[0, s] += wre * tx[:, ny:] - wim * tx[:, :ny]
            plane_sum[1, s] += wre * ty[nx:] - wim * ty[:nx]
        return carry

    lax.fori_loop(0, bands, lateral, 0)

    def to_peer(k):
        peer = lax.rem(b + k, nb)
        return pltpu.make_async_remote_copy(
            src_ref=plane_sum.at[:, :, pl.ds(pl.multiple_of(peer * rows, rows), rows), :],
            dst_ref=plane_recv.at[k - 1],
            send_sem=plane_send_sem.at[k - 1],
            recv_sem=plane_recv_sem.at[k - 1],
            device_id={"band": peer, "grid": g},
        )

    for k in range(1, nb):
        to_peer(k).start()

    for k in range(chips):
        to_mate(k).wait_recv()
        to_inner(k).start()

    mine = pl.ds(pl.multiple_of(b * rows, rows), rows)
    summed = plane_sum[:, :, mine, :]
    for k in range(1, nb):
        to_peer(k).wait_recv()
        summed = summed + plane_recv[k - 1]
    out_ref[1:3] = summed * (1.0 / 12.0)

    def depthwise(k):
        direct = k >= chips
        first = odd if direct else 1 - odd
        second = 1 - first
        sign = (turn if direct else -turn).astype(jnp.float32)
        start = start_of(k, odd)

        def at_home(n, q, p):
            return own[n, q, p, pl.ds(start, half), :].astype(jnp.float32)

        def at_mate(n, q, p):
            return mate[k, n, q, p].astype(jnp.float32)

        def at_far(n, q, p):
            return (outer[k - chips, n, q, p] if direct else inner[k, n, q, p]).astype(jnp.float32)

        chain = (at_home, at_mate, at_far) if direct else (at_mate, at_home, at_far)

        def step(n, sums):
            w = occ_ref[n] * sign
            fields = [tuple(held(n, q, p) for q in (0, 1)) for held in chain for p in (first, second)]
            scaled = [(re * w, im * w) for re, im in fields[:4]]
            return tuple(
                total + (scaled[i][0] * fields[j][1] - scaled[i][1] * fields[j][0])
                for total, (i, j) in zip(sums, PAIRS)
            )

        zero = jnp.zeros((half, ny), jnp.float32)
        n01, n12, n23, n34, f02, f13, f24, f35 = lax.fori_loop(0, bands, step, (zero,) * 8, unroll=4)
        parts = (
            (8.0 * n01 - f02, 8.0 * (n01 + n12) - f13),
            (8.0 * (n12 + n23) - f02 - f24, 8.0 * (n23 + n34) - f13 - f35),
            (8.0 * n34 - f24, -f35),
        )
        for role, part in enumerate(parts if direct else (parts[1], parts[0], parts[2])):
            zsend[k, role, first] = part[0]
            zsend[k, role, second] = part[1]

    def to_inbox(k):
        chunk = chunk_of(k)
        slot = lax.rem(b - 2 * (chunk // 2) - 2 + nb, nb)
        return pltpu.make_async_remote_copy(
            src_ref=zsend.at[k],
            dst_ref=inbox.at[slot],
            send_sem=inbox_send.at[k],
            recv_sem=inbox_recv.at[slot],
            device_id={"band": chunk, "grid": g},
        )

    def from_inbox(slot):
        return pltpu.make_async_remote_copy(
            src_ref=zsend.at[0],
            dst_ref=inbox.at[slot],
            send_sem=inbox_send.at[0],
            recv_sem=inbox_recv.at[slot],
            device_id={"band": b, "grid": partner},
        )

    def to_final(k, role):
        slot = (0, 1 + core, 3 + core)[role]
        at = (g, partner, ahead if k >= chips else side)[role]
        return pltpu.make_async_remote_copy(
            src_ref=zsend.at[k, role],
            dst_ref=final.at[slot],
            send_sem=final_send.at[k // chips, role],
            recv_sem=final_recv.at[slot],
            device_id={"band": 2 * chip + k // chips, "grid": at},
        )

    def from_final(slot):
        return pltpu.make_async_remote_copy(
            src_ref=zsend.at[0, 0],
            dst_ref=final.at[slot],
            send_sem=final_send.at[0, 0],
            recv_sem=final_recv.at[slot],
            device_id={"band": b, "grid": partner},
        )

    def arrive(k):
        to_mate(k).wait_recv()
        to_outer(k).wait_recv()

    def finish(k):
        kind = k // chips

        @pl.when(core == kind)
        def _():
            for slot in range(nb - 2):
                from_inbox(slot).wait_recv()
            zsend[k] = zsend[k] + sum(inbox[slot] for slot in range(nb - 2))

        @pl.when(core != kind)
        def _():
            to_final(k, 0).start()

        for role in (2, 1):
            to_final(k, role).start()

    for j in range(chips - 1):
        arrive(chips + j)
        depthwise(chips + j)
        to_inbox(chips + j).start()
        to_inner(j).wait_recv()
        depthwise(j)
        to_inbox(j).start()
    arrive(nb - 1)
    depthwise(nb - 1)
    finish(nb - 1)
    to_inner(chips - 1).wait_recv()
    depthwise(chips - 1)
    finish(chips - 1)

    near = pl.ds(pl.multiple_of(odd * half, half), half)
    away = pl.ds(pl.multiple_of((1 - odd) * half, half), half)
    for slot in range(5):
        from_final(slot).wait_recv()
    far = final[3] + final[4]
    home = final[0]
    across = final[1] + final[2]

    @pl.when(core == 1)
    def _():
        out_ref[0, :, near, :] = (zsend[nb - 1, 0] + home + far) * (1.0 / 12.0)
        out_ref[0, :, away, :] = across * (1.0 / 12.0)

    @pl.when(core == 0)
    def _():
        out_ref[0, :, near, :] = (zsend[chips - 1, 0] + home) * (1.0 / 12.0)
        out_ref[0, :, away, :] = (across + far) * (1.0 / 12.0)

    for k in range(1, nb):
        to_peer(k).wait_send()
    for k in range(nb):
        to_mate(k).wait_send()
    for k in range(chips):
        to_outer(chips + k).wait_send()
        to_inner(k).wait_send()
    for k in range(chips - 1):
        to_inbox(k).wait_send()
        to_inbox(chips + k).wait_send()
    for k in (chips - 1, nb - 1):
        to_final(k, 1).wait_send()
        to_final(k, 2).wait_send()

        @pl.when(core != k // chips)
        def _():
            to_final(k, 0).wait_send()


def solution(mesh):
    nb = mesh.shape["band"]
    ng = mesh.shape["grid"]

    def per_device(orbitals, occupations):
        bands, _, depth, nx, ny = orbitals.shape
        rows = nx // nb
        half = rows // 2
        if depth != 2 or nb % 2 or nb < 4 or ng % 2 or ng < 6 or half % TILE:
            raise ValueError("unsupported sizes")
        chips = nb // 2
        f32, bf16 = jnp.float32, jnp.bfloat16
        dma = pltpu.SemaphoreType.DMA
        return pl.pallas_call(
            functools.partial(kernel, nb, ng),
            out_shape=jax.ShapeDtypeStruct((3, depth, rows, ny), f32),
            in_specs=[
                pl.BlockSpec(memory_space=pltpu.HBM),
                pl.BlockSpec(memory_space=pltpu.HBM),
            ],
            out_specs=pl.BlockSpec(memory_space=pltpu.VMEM),
            scratch_shapes=[
                pltpu.SMEM((bands,), f32),
                pltpu.VMEM((bands, 2, depth, nx, ny), bf16),
                pltpu.VMEM((nb, bands, 2, depth, half, ny), bf16),
                pltpu.VMEM((chips, bands, 2, depth, half, ny), bf16),
                pltpu.VMEM((chips, bands, 2, depth, half, ny), bf16),
                pltpu.VMEM((nx, nx), bf16),
                pltpu.VMEM((ny, ny), bf16),
                pltpu.VMEM((2, depth, nx, ny), f32),
                pltpu.VMEM((nb - 1, 2, depth, rows, ny), f32),
                pltpu.VMEM((nb, 3, depth, half, ny), f32),
                pltpu.VMEM((nb - 2, 3, depth, half, ny), f32),
                pltpu.VMEM((5, depth, half, ny), f32),
                dma,
                dma,
                dma((nb,)),
                dma((nb,)),
                dma((chips,)),
                dma((chips,)),
                dma((chips,)),
                dma((chips,)),
                dma((nb - 1,)),
                dma((nb - 1,)),
                dma((nb,)),
                dma((nb - 2,)),
                dma((2, 3)),
                dma((5,)),
                pltpu.SemaphoreType.REGULAR,
                pltpu.SemaphoreType.REGULAR,
            ],
            compiler_params=pltpu.CompilerParams(collective_id=0, has_side_effects=True, vmem_limit_bytes=55000 * 1024),
            name="current",
        )(occupations, orbitals)

    return jax.shard_map(
        per_device,
        mesh=mesh,
        in_specs=(P("band", None, "grid", None, None), P("band")),
        out_specs=P(None, "grid", "band", None),
        check_vma=False,
    )
```

```python
import functools

import jax
import jax.numpy as jnp
from jax import lax
from jax.experimental import pallas as pl
from jax.experimental.pallas import tpu as pltpu
from jax.sharding import PartitionSpec as P

TILE = 16
PAIRS = ((0, 1), (1, 2), (2, 3), (3, 4), (0, 2), (1, 3), (2, 4), (3, 5))


def stencil(n, flipped):
    row = lax.broadcasted_iota(jnp.int32, (n, n), 0)
    col = lax.broadcasted_iota(jnp.int32, (n, n), 1)
    d = col - row if flipped else row - col
    value = jnp.zeros((n, n), jnp.float32)
    for step, weight in ((1, 8.0), (-1, -8.0), (2, -1.0), (-2, 1.0)):
        hit = (d == step) | (d == step - n) | (d == step + n)
        value = jnp.where(hit, weight, value)
    return value.astype(jnp.bfloat16)


def kernel(
    nb, ng, occ_hbm, orb_ref, out_ref,
    occ_ref, own, mate, outer, inner, mx, my, plane_sum, plane_recv, zsend, inbox, final,
    occ_sem, own_sem, mate_send, mate_recv, outer_send, outer_recv, inner_send, inner_recv,
    plane_send_sem, plane_recv_sem, inbox_send, inbox_recv, final_send, last_send, final_recv, up_token, down_token,
):
    bands, _, depth, nx, ny = orb_ref.shape
    b = lax.axis_index("band")
    g = lax.axis_index("grid")
    odd = lax.rem(g, 2)
    turn = 1 - 2 * odd
    partner = g + turn
    ahead = lax.rem(g + 2 * turn + ng, ng)
    behind = lax.rem(g - 2 * turn + ng, ng)
    side = lax.rem(g - turn + ng, ng)
    layers = ng // 2
    layer = g // 2
    rows = nx // nb
    half = rows // 2
    chips = nb // 2
    chip = b // 2
    core = lax.rem(b, 2)
    split = bands // 2

    load = pltpu.make_async_copy(orb_ref, own, own_sem)
    load.start()
    weights = pltpu.make_async_copy(occ_hbm, occ_ref, occ_sem)
    weights.start()

    barrier = pltpu.get_barrier_semaphore()
    peers = [lax.rem(b + k, nb) for k in range(1, nb)]
    pl.semaphore_signal(barrier, inc=1, device_id={"band": b, "grid": partner})
    for peer in peers:
        pl.semaphore_signal(barrier, inc=1, device_id={"band": peer, "grid": g})

    @pl.when(layer > 0)
    def _():
        pl.semaphore_signal(barrier, inc=1, device_id={"band": b, "grid": g - 2})

    @pl.when(layer < layers - 1)
    def _():
        pl.semaphore_signal(barrier, inc=1, device_id={"band": b, "grid": g + 2})

    ends = (layer == 0).astype(jnp.int32) + (layer == layers - 1).astype(jnp.int32)
    pl.semaphore_wait(barrier, nb + 2 - ends)

    def chunk_of(j):
        return 2 * lax.rem(chip + 1 + j // 2, chips) + j % 2

    def rows_of(j, parity):
        return pl.ds(pl.multiple_of(chunk_of(j) * rows + parity * half, half), half)

    passed, straight = pl.ds(0, split), pl.ds(split, bands - split)

    def to_mate(j, kind):
        part = (passed, straight)[kind]
        return pltpu.make_async_remote_copy(
            src_ref=orb_ref.at[part, :, :, rows_of(j, 1 - odd), :],
            dst_ref=mate.at[j, part],
            send_sem=mate_send.at[kind, j],
            recv_sem=mate_recv.at[kind, j],
            device_id={"band": b, "grid": partner},
        )

    def to_outer(j, source):
        return pltpu.make_async_remote_copy(
            src_ref=source.at[straight, :, :, rows_of(j, odd), :],
            dst_ref=outer.at[j],
            send_sem=outer_send.at[j],
            recv_sem=outer_recv.at[j],
            device_id={"band": b, "grid": behind},
        )

    def to_inner(j):
        return pltpu.make_async_remote_copy(
            src_ref=mate.at[j, passed],
            dst_ref=inner.at[j],
            send_sem=inner_send.at[j],
            recv_sem=inner_recv.at[j],
            device_id={"band": b, "grid": ahead},
        )

    wraps = ((odd == 0) & (layer == 0)) | ((odd == 1) & (layer == layers - 1))
    for kind in (0, 1):
        for j in range(nb):
            to_mate(j, kind).start()

    @pl.when(jnp.logical_not(wraps))
    def _():
        for j in range(nb):
            to_outer(j, orb_ref).start()

    @pl.when(layer == 1)
    def _():
        pl.semaphore_signal(up_token, inc=1, device_id={"band": b, "grid": g + 2})

    @pl.when(layer == layers - 2)
    def _():
        pl.semaphore_signal(down_token, inc=1, device_id={"band": b, "grid": g - 2})

    @pl.when(layer >= 2)
    def _():
        pl.semaphore_wait(up_token, 1)

        @pl.when(layer < layers - 1)
        def _():
            pl.semaphore_signal(up_token, inc=1, device_id={"band": b, "grid": g + 2})

    @pl.when(layer <= layers - 3)
    def _():
        pl.semaphore_wait(down_token, 1)

        @pl.when(layer > 0)
        def _():
            pl.semaphore_signal(down_token, inc=1, device_id={"band": b, "grid": g - 2})

    load.wait()

    @pl.when(wraps)
    def _():
        for j in range(nb):
            to_outer(j, own).start()

    mx[...] = stencil(nx, True)
    my[...] = stencil(ny, False)
    plane_sum[...] = jnp.zeros_like(plane_sum)
    weights.wait()

    def lateral(n, carry):
        w = occ_ref[n]
        for s in range(depth):
            re = own[n, 0, s]
            im = own[n, 1, s]
            tx = jnp.dot(mx[...], jnp.concatenate([re, im], 1), preferred_element_type=jnp.float32)
            ty = jnp.dot(jnp.concatenate([re, im], 0), my[...], preferred_element_type=jnp.float32)
            wre = re.astype(jnp.float32) * w
            wim = im.astype(jnp.float32) * w
            plane_sum[0, s] += wre * tx[:, ny:] - wim * tx[:, :ny]
            plane_sum[1, s] += wre * ty[nx:] - wim * ty[:nx]
        return carry

    lax.fori_loop(0, bands, lateral, 0)

    def to_peer(k):
        peer = lax.rem(b + k, nb)
        return pltpu.make_async_remote_copy(
            src_ref=plane_sum.at[:, :, pl.ds(pl.multiple_of(peer * rows, rows), rows), :],
            dst_ref=plane_recv.at[k - 1],
            send_sem=plane_send_sem.at[k - 1],
            recv_sem=plane_recv_sem.at[k - 1],
            device_id={"band": peer, "grid": g},
        )

    for k in range(1, nb):
        to_peer(k).start()

    for j in range(nb):
        to_mate(j, 0).wait_recv()
        to_inner(j).start()

    mine = pl.ds(pl.multiple_of(b * rows, rows), rows)
    summed = plane_sum[:, :, mine, :]
    for k in range(1, nb):
        to_peer(k).wait_recv()
        summed = summed + plane_recv[k - 1]
    out_ref[1:3] = summed * (1.0 / 12.0)

    def depthwise(j, kind):
        first = odd if kind else 1 - odd
        second = 1 - first
        sign = (turn if kind else -turn).astype(jnp.float32)
        here = rows_of(j, odd)

        def at_home(n, q, p):
            return own[n, q, p, here, :].astype(jnp.float32)

        def at_mate(n, q, p):
            return mate[j, n, q, p].astype(jnp.float32)

        def at_far(n, q, p):
            return (outer[j, n - split, q, p] if kind else inner[j, n, q, p]).astype(jnp.float32)

        chain = (at_home, at_mate, at_far) if kind else (at_mate, at_home, at_far)

        def step(n, sums):
            w = occ_ref[n] * sign
            fields = [tuple(held(n, q, p) for q in (0, 1)) for held in chain for p in (first, second)]
            scaled = [(re * w, im * w) for re, im in fields[:4]]
            return tuple(
                total + (scaled[i][0] * fields[k][1] - scaled[i][1] * fields[k][0])
                for total, (i, k) in zip(sums, PAIRS)
            )

        zero = jnp.zeros((half, ny), jnp.float32)
        span = (split, bands) if kind else (0, split)
        n01, n12, n23, n34, f02, f13, f24, f35 = lax.fori_loop(*span, step, (zero,) * 8, unroll=4)
        parts = (
            (8.0 * n01 - f02, 8.0 * (n01 + n12) - f13),
            (8.0 * (n12 + n23) - f02 - f24, 8.0 * (n23 + n34) - f13 - f35),
            (8.0 * n34 - f24, -f35),
        )
        if kind:
            for role in range(3):
                zsend[j, role, first] = parts[role][0]
                zsend[j, role, second] = parts[role][1]
        else:
            for role in range(2):
                zsend[j, role, first] += parts[1 - role][0]
                zsend[j, role, second] += parts[1 - role][1]
            zsend[j, 3, first] = parts[2][0]
            zsend[j, 3, second] = parts[2][1]

    def to_inbox(j):
        chunk = chunk_of(j)
        slot = lax.rem(b - 2 * (chunk // 2) - 2 + nb, nb)
        return pltpu.make_async_remote_copy(
            src_ref=zsend.at[j],
            dst_ref=inbox.at[slot],
            send_sem=inbox_send.at[j],
            recv_sem=inbox_recv.at[slot],
            device_id={"band": chunk, "grid": g},
        )

    def from_inbox(slot):
        return pltpu.make_async_remote_copy(
            src_ref=zsend.at[0],
            dst_ref=inbox.at[slot],
            send_sem=inbox_send.at[0],
            recv_sem=inbox_recv.at[slot],
            device_id={"band": b, "grid": partner},
        )

    def to_final(j, role):
        slot = 2 * role - 1 + core if role else 0
        at = (g, partner, ahead, side)[role]
        return pltpu.make_async_remote_copy(
            src_ref=zsend.at[j, role],
            dst_ref=final.at[slot],
            send_sem=final_send.at[role],
            recv_sem=final_recv.at[slot],
            device_id={"band": 2 * chip + j % 2, "grid": at},
        )

    def to_last(role):
        slot = 2 * role - 1 + core if role else 0
        return pltpu.make_async_remote_copy(
            src_ref=zsend.at[nb - 1, role],
            dst_ref=final.at[slot],
            send_sem=last_send.at[role],
            recv_sem=final_recv.at[slot],
            device_id={"band": 2 * chip + 1, "grid": (g, partner, ahead, side)[role]},
        )

    def from_final(slot):
        return pltpu.make_async_remote_copy(
            src_ref=zsend.at[0, 0],
            dst_ref=final.at[slot],
            send_sem=final_send.at[0],
            recv_sem=final_recv.at[slot],
            device_id={"band": b, "grid": partner},
        )

    def straight_part(j):
        to_mate(j, 1).wait_recv()
        to_outer(j, orb_ref).wait_recv()
        depthwise(j, 1)

    def passed_part(j):
        to_inner(j).wait_recv()
        depthwise(j, 0)

    others = range(nb - 2)
    for j in range(nb - 2):
        straight_part(j)
        passed_part(j)
        to_inbox(j).start()

    straight_part(nb - 2)
    passed_part(nb - 2)

    @pl.when(core == 1)
    def _():
        to_inbox(nb - 2).start()

    @pl.when(core == 0)
    def _():
        for slot in (*others, nb - 1):
            from_inbox(slot).wait_recv()
        zsend[nb - 2] = zsend[nb - 2] + inbox[nb - 1] + sum(inbox[slot] for slot in others)
        for role in (2, 3, 1):
            to_final(nb - 2, role).start()

    straight_part(nb - 1)

    @pl.when(core == 1)
    def _():
        for slot in others:
            from_inbox(slot).wait_recv()
        zsend[nb - 1, :3] = zsend[nb - 1, :3] + sum(inbox[slot, :3] for slot in others)
        to_final(nb - 1, 2).start()

    @pl.when(core == 0)
    def _():
        to_last(2).start()

    passed_part(nb - 1)

    @pl.when(core == 1)
    def _():
        zsend[nb - 1, 3] = zsend[nb - 1, 3] + sum(inbox[slot, 3] for slot in others)
        for role in (3, 1):
            to_final(nb - 1, role).start()

    @pl.when(core == 0)
    def _():
        for role in (3, 1, 0):
            to_last(role).start()

    near = pl.ds(pl.multiple_of(odd * half, half), half)
    away = pl.ds(pl.multiple_of((1 - odd) * half, half), half)

    @pl.when(core == 1)
    def _():
        for slot in range(7):
            from_final(slot).wait_recv()
        out_ref[0, :, near, :] = (zsend[nb - 1, 0] + final[0] + final[3] + final[4]) * (1.0 / 12.0)
        out_ref[0, :, away, :] = (final[1] + final[2] + final[5] + final[6]) * (1.0 / 12.0)

    @pl.when(core == 0)
    def _():
        for slot in (1, 3, 5):
            from_final(slot).wait_recv()
        out_ref[0, :, near, :] = (zsend[nb - 2, 0] + final[3]) * (1.0 / 12.0)
        out_ref[0, :, away, :] = (final[1] + final[5]) * (1.0 / 12.0)

    for k in range(1, nb):
        to_peer(k).wait_send()
    for j in range(nb):
        to_mate(j, 0).wait_send()
        to_mate(j, 1).wait_send()
        to_outer(j, orb_ref).wait_send()
        to_inner(j).wait_send()
    for j in range(nb - 2):
        to_inbox(j).wait_send()

    @pl.when(core == 1)
    def _():
        to_inbox(nb - 2).wait_send()
        for role in (1, 2, 3):
            to_final(nb - 1, role).wait_send()

    @pl.when(core == 0)
    def _():
        for role in (1, 2, 3):
            to_final(nb - 2, role).wait_send()
        for role in range(4):
            to_last(role).wait_send()


def solution(mesh):
    nb = mesh.shape["band"]
    ng = mesh.shape["grid"]

    def per_device(orbitals, occupations):
        bands, _, depth, nx, ny = orbitals.shape
        rows = nx // nb
        half = rows // 2
        if depth != 2 or nb % 2 or nb < 4 or ng % 2 or ng < 6 or half % TILE:
            raise ValueError("unsupported sizes")
        f32, bf16 = jnp.float32, jnp.bfloat16
        dma = pltpu.SemaphoreType.DMA
        return pl.pallas_call(
            functools.partial(kernel, nb, ng),
            out_shape=jax.ShapeDtypeStruct((3, depth, rows, ny), f32),
            in_specs=[
                pl.BlockSpec(memory_space=pltpu.HBM),
                pl.BlockSpec(memory_space=pltpu.HBM),
            ],
            out_specs=pl.BlockSpec(memory_space=pltpu.VMEM),
            scratch_shapes=[
                pltpu.SMEM((bands,), f32),
                pltpu.VMEM((bands, 2, depth, nx, ny), bf16),
                pltpu.VMEM((nb, bands, 2, depth, half, ny), bf16),
                pltpu.VMEM((nb, bands - bands // 2, 2, depth, half, ny), bf16),
                pltpu.VMEM((nb, bands // 2, 2, depth, half, ny), bf16),
                pltpu.VMEM((nx, nx), bf16),
                pltpu.VMEM((ny, ny), bf16),
                pltpu.VMEM((2, depth, nx, ny), f32),
                pltpu.VMEM((nb - 1, 2, depth, rows, ny), f32),
                pltpu.VMEM((nb, 4, depth, half, ny), f32),
                pltpu.VMEM((nb, 4, depth, half, ny), f32),
                pltpu.VMEM((7, depth, half, ny), f32),
                dma,
                dma,
                dma((2, nb)),
                dma((2, nb)),
                dma((nb,)),
                dma((nb,)),
                dma((nb,)),
                dma((nb,)),
                dma((nb - 1,)),
                dma((nb - 1,)),
                dma((nb,)),
                dma((nb,)),
                dma((4,)),
                dma((4,)),
                dma((7,)),
                pltpu.SemaphoreType.REGULAR,
                pltpu.SemaphoreType.REGULAR,
            ],
            compiler_params=pltpu.CompilerParams(collective_id=0, has_side_effects=True, vmem_limit_bytes=55000 * 1024),
            name="current",
        )(pltpu.with_memory_space_constraint(occupations, pltpu.HBM), orbitals)

    return jax.shard_map(
        per_device,
        mesh=mesh,
        in_specs=(P("band", None, "grid", None, None), P("band")),
        out_specs=P(None, "grid", "band", None),
        check_vma=False,
    )
```

```python
import functools

import jax
import jax.numpy as jnp
from jax import lax
from jax.experimental import pallas as pl
from jax.experimental.pallas import tpu as pltpu
from jax.sharding import PartitionSpec as P

TILE = 16
MIXED = ()
HELD = 0


def stencil(n, flipped):
    row = lax.broadcasted_iota(jnp.int32, (n, n), 0)
    col = lax.broadcasted_iota(jnp.int32, (n, n), 1)
    d = col - row if flipped else row - col
    value = jnp.zeros((n, n), jnp.float32)
    for step, weight in ((1, 8.0), (-1, -8.0), (2, -1.0), (-2, 1.0)):
        hit = (d == step) | (d == step - n) | (d == step + n)
        value = jnp.where(hit, weight, value)
    return value.astype(jnp.bfloat16)


def kernel(
    nb, ng, occ_hbm, orb_ref, out_ref,
    occ_ref, own, mate, outer, inner, mx, my, plane_sum, plane_recv, zsend, inbox, final,
    occ_sem, own_sem, mate_send, mate_recv, outer_send, outer_recv, inner_send, inner_recv,
    plane_send_sem, plane_recv_sem, inbox_send, inbox_recv, final_send, final_recv, up_token, down_token,
):
    bands, _, depth, nx, ny = orb_ref.shape
    b = lax.axis_index("band")
    g = lax.axis_index("grid")
    odd = lax.rem(g, 2)
    turn = 1 - 2 * odd
    partner = g + turn
    ahead = lax.rem(g + 2 * turn + ng, ng)
    behind = lax.rem(g - 2 * turn + ng, ng)
    side = lax.rem(g - turn + ng, ng)
    layers = ng // 2
    layer = g // 2
    rows = nx // nb
    half = rows // 2
    split = bands // 2
    relayed = nb // 2

    load = pltpu.make_async_copy(orb_ref, own, own_sem)
    load.start()
    weights = pltpu.make_async_copy(occ_hbm, occ_ref, occ_sem)
    weights.start()

    barrier = pltpu.get_barrier_semaphore()
    peers = [lax.rem(b + k, nb) for k in range(1, nb)]
    pl.semaphore_signal(barrier, inc=1, device_id={"band": b, "grid": partner})
    for peer in peers:
        pl.semaphore_signal(barrier, inc=1, device_id={"band": peer, "grid": g})

    @pl.when(layer > 0)
    def _():
        pl.semaphore_signal(barrier, inc=1, device_id={"band": b, "grid": g - 2})

    @pl.when(layer < layers - 1)
    def _():
        pl.semaphore_signal(barrier, inc=1, device_id={"band": b, "grid": g + 2})

    ends = (layer == 0).astype(jnp.int32) + (layer == layers - 1).astype(jnp.int32)
    pl.semaphore_wait(barrier, nb + 2 - ends)

    def rows_of(j, parity):
        return pl.ds(pl.multiple_of(j * rows + parity * half, half), half)

    passed, straight = pl.ds(0, split), pl.ds(split, bands - split)
    mixed = [j for j in MIXED if j < nb]
    last_passed = [split - (j in mixed) for j in range(nb)]

    def to_mate(j, kind):
        part = (passed, straight)[kind]
        return pltpu.make_async_remote_copy(
            src_ref=orb_ref.at[part, :, :, rows_of(j, 1 - odd), :],
            dst_ref=mate.at[j, part],
            send_sem=mate_send.at[kind, j],
            recv_sem=mate_recv.at[kind, j],
            device_id={"band": b, "grid": partner},
        )

    def to_outer(j, source):
        return pltpu.make_async_remote_copy(
            src_ref=source.at[straight, :, :, rows_of(j, odd), :],
            dst_ref=outer.at[j, pl.ds(1, bands - split)],
            send_sem=outer_send.at[0, j],
            recv_sem=outer_recv.at[0, j],
            device_id={"band": b, "grid": behind},
        )

    def to_outer_mixed(j):
        return pltpu.make_async_remote_copy(
            src_ref=orb_ref.at[split - 1, :, :, rows_of(j, odd), :],
            dst_ref=outer.at[j, 0],
            send_sem=outer_send.at[1, j],
            recv_sem=outer_recv.at[1, j],
            device_id={"band": b, "grid": behind},
        )

    def to_inner(j):
        return pltpu.make_async_remote_copy(
            src_ref=mate.at[j, pl.ds(0, last_passed[j])],
            dst_ref=inner.at[j, pl.ds(0, last_passed[j])],
            send_sem=inner_send.at[0, j],
            recv_sem=inner_recv.at[0, j],
            device_id={"band": b, "grid": ahead},
        )

    def to_inner_mixed(j):
        return pltpu.make_async_remote_copy(
            src_ref=mate.at[j, split - 1],
            dst_ref=inner.at[j, split - 1],
            send_sem=inner_send.at[1, j],
            recv_sem=inner_recv.at[1, j],
            device_id={"band": b, "grid": ahead},
        )

    wraps = ((odd == 0) & (layer == 0)) | ((odd == 1) & (layer == layers - 1))
    wraps_ahead = ((odd == 0) & (layer == layers - 1)) | ((odd == 1) & (layer == 0))
    for kind in (0, 1):
        for j in range(nb):
            to_mate(j, kind).start()

    @pl.when(jnp.logical_not(wraps))
    def _():
        for j in range(nb - HELD):
            to_outer(j, orb_ref).start()
        for j in mixed:
            to_outer_mixed(j).start()

    @pl.when(layer == 1)
    def _():
        pl.semaphore_signal(up_token, inc=1, device_id={"band": b, "grid": g + 2})

    @pl.when(layer == layers - 2)
    def _():
        pl.semaphore_signal(down_token, inc=1, device_id={"band": b, "grid": g - 2})

    @pl.when(layer >= 2)
    def _():
        pl.semaphore_wait(up_token, 1)

        @pl.when(layer < layers - 1)
        def _():
            pl.semaphore_signal(up_token, inc=1, device_id={"band": b, "grid": g + 2})

    @pl.when(layer <= layers - 3)
    def _():
        pl.semaphore_wait(down_token, 1)

        @pl.when(layer > 0)
        def _():
            pl.semaphore_signal(down_token, inc=1, device_id={"band": b, "grid": g - 2})

    load.wait()

    @pl.when(wraps)
    def _():
        for j in range(nb):
            to_outer(j, own).start()

    mx[...] = stencil(nx, True)
    my[...] = stencil(ny, False)
    plane_sum[...] = jnp.zeros_like(plane_sum)
    weights.wait()

    def lateral(n, carry):
        w = occ_ref[n]
        for s in range(depth):
            re = own[n, 0, s]
            im = own[n, 1, s]
            tx = jnp.dot(mx[...], jnp.concatenate([re, im], 1), preferred_element_type=jnp.float32)
            ty = jnp.dot(jnp.concatenate([re, im], 0), my[...], preferred_element_type=jnp.float32)
            wre = re.astype(jnp.float32) * w
            wim = im.astype(jnp.float32) * w
            plane_sum[0, s] += wre * tx[:, ny:] - wim * tx[:, :ny]
            plane_sum[1, s] += wre * ty[nx:] - wim * ty[:nx]
        return carry

    lax.fori_loop(0, bands, lateral, 0)

    def to_peer(k):
        peer = lax.rem(b + k, nb)
        return pltpu.make_async_remote_copy(
            src_ref=plane_sum.at[:, :, pl.ds(pl.multiple_of(peer * rows, rows), rows), :],
            dst_ref=plane_recv.at[k - 1],
            send_sem=plane_send_sem.at[k - 1],
            recv_sem=plane_recv_sem.at[k - 1],
            device_id={"band": peer, "grid": g},
        )

    for k in range(1, nb):
        to_peer(k).start()

    for j in range(nb):
        to_mate(j, 0).wait_recv()
        to_inner(j).start()
        if j in mixed:
            @pl.when(wraps_ahead)
            def _():
                to_inner_mixed(j).start()

    @pl.when(jnp.logical_not(wraps))
    def _():
        for j in range(nb - HELD, nb):
            to_outer(j, own).start()

    mine = pl.ds(pl.multiple_of(b * rows, rows), rows)
    summed = plane_sum[:, :, mine, :]
    for k in range(1, nb):
        to_peer(k).wait_recv()
        summed = summed + plane_recv[k - 1]
    out_ref[1:3] = summed * (1.0 / 12.0)

    first = odd
    second = 1 - odd
    sign = turn.astype(jnp.float32)
    zero = jnp.zeros((half, ny), jnp.float32)

    def fields_of(held, n):
        return [tuple(held(n, q, p) for q in (0, 1)) for p in (first, second)]

    def bonds(n, low, high, sums):
        w = occ_ref[n] * sign
        low = [(re * w, im * w) for re, im in low]
        pairs = ((1, 0), (0, 0), (1, 1))
        return tuple(
            total + (low[i][0] * high[k][1] - low[i][1] * high[k][0]) for total, (i, k) in zip(sums, pairs)
        )

    def at_home(j):
        return lambda n, q, p: own[n, q, p, rows_of(j, odd), :].astype(jnp.float32)

    def at_mate(j):
        return lambda n, q, p: mate[j, n, q, p].astype(jnp.float32)

    def core_part(j):
        def step(n, sums):
            low, high = fields_of(at_home(j), n), fields_of(at_mate(j), n)
            w = occ_ref[n] * sign
            inside = tuple(
                total + (slab[0][0] * w * slab[1][1] - slab[0][1] * w * slab[1][0])
                for total, slab in zip(sums[3:], (low, high))
            )
            return bonds(n, low, high, sums[:3]) + inside

        n12, f02, f13, n01, n23 = lax.fori_loop(0, bands, step, (zero,) * 5, unroll=4)
        zsend[j, 0, first] = 8.0 * n01 - f02
        zsend[j, 0, second] = 8.0 * (n01 + n12) - f13
        zsend[j, 1, first] = 8.0 * (n12 + n23) - f02
        zsend[j, 1, second] = 8.0 * n23 - f13

    def straight_part(j):
        def step(n, sums):
            far = fields_of(lambda n, q, p: outer[j, n - split + 1, q, p].astype(jnp.float32), n)
            return bonds(n, fields_of(at_mate(j), n), far, sums)

        sums = lax.fori_loop(split, bands, step, (zero,) * 3, unroll=True)
        if j in mixed:
            sums = lax.fori_loop(split - jnp.where(wraps_ahead, 0, 1), split, step, sums)
        n34, f24, f35 = sums
        zsend[j, 1, first] += -f24
        zsend[j, 1, second] += 8.0 * n34 - f35
        zsend[j, 2, first] = 8.0 * n34 - f24
        zsend[j, 2, second] = -f35

    def passed_part(j):
        def step(n, sums):
            far = fields_of(lambda n, q, p: inner[j, n, q, p].astype(jnp.float32), n)
            return bonds(n, far, fields_of(at_home(j), n), sums)

        sums = lax.fori_loop(0, last_passed[j], step, (zero,) * 3, unroll=True)
        if j in mixed:
            sums = lax.fori_loop(split - jnp.where(wraps, 1, 0), split, step, sums)
        n10, f20, f11 = sums
        zsend[j, 0, first] += 8.0 * n10 - f20
        zsend[j, 0, second] += -f11
        zsend[j, 3, first] = -f20
        zsend[j, 3, second] = 8.0 * n10 - f11

    def to_inbox(j):
        slot = lax.rem(b - j - 1 + nb, nb)
        return pltpu.make_async_remote_copy(
            src_ref=zsend.at[j],
            dst_ref=inbox.at[slot],
            send_sem=inbox_send.at[j],
            recv_sem=inbox_recv.at[slot],
            device_id={"band": j, "grid": g},
        )

    def from_inbox(slot):
        return pltpu.make_async_remote_copy(
            src_ref=zsend.at[0],
            dst_ref=inbox.at[slot],
            send_sem=inbox_send.at[0],
            recv_sem=inbox_recv.at[slot],
            device_id={"band": b, "grid": partner},
        )

    def to_final(j, role):
        return pltpu.make_async_remote_copy(
            src_ref=zsend.at[j, role],
            dst_ref=final.at[role, b],
            send_sem=final_send.at[j, role],
            recv_sem=final_recv.at[role, b],
            device_id={"band": j, "grid": (g, partner, ahead, side)[role]},
        )

    def from_final(role, source):
        return pltpu.make_async_remote_copy(
            src_ref=zsend.at[0, 0],
            dst_ref=final.at[role, source],
            send_sem=final_send.at[0, 0],
            recv_sem=final_recv.at[role, source],
            device_id={"band": b, "grid": partner},
        )

    def arrive_mate(j):
        to_mate(j, 1).wait_recv()

    def arrive_outer(j):
        to_outer(j, own).wait_recv()
        if j in mixed:
            @pl.when(jnp.logical_not(wraps_ahead))
            def _():
                to_outer_mixed(j).wait_recv()

    def arrive_inner(j):
        to_inner(j).wait_recv()
        if j in mixed:
            @pl.when(wraps)
            def _():
                to_inner_mixed(j).wait_recv()

    def finish(j):
        @pl.when(b == j)
        def _():
            for slot in range(nb - 1):
                from_inbox(slot).wait_recv()
            zsend[j] = zsend[j] + sum(inbox[slot] for slot in range(nb - 1))
            for role in (3, 2, 1):
                to_final(j, role).start()

    for j in range(relayed):
        arrive_mate(j)
        core_part(j)
        arrive_outer(j)
        straight_part(j)
        arrive_inner(j)
        passed_part(j)

        @pl.when(b != j)
        def _():
            to_inbox(j).start()

        if j:
            finish(j - 1)

    def straight_last(j, mate_too):
        arrive_outer(j)
        straight_part(j)
        to_final(j, 2).start()
        if mate_too:
            to_final(j, 1).start()

    def passed_last(j):
        arrive_inner(j)
        passed_part(j)
        to_final(j, 3).start()

        @pl.when(b != j)
        def _():
            to_final(j, 0).start()

    for j in range(relayed, nb - 1):
        arrive_mate(j)
        if j > relayed:
            to_final(j - 1, 1).start()
        core_part(j)
        straight_last(j, False)
        if j == relayed:
            finish(relayed - 1)
        passed_last(j)

    arrive_mate(nb - 1)
    to_final(nb - 2, 1).start()
    core_part(nb - 1)

    @pl.when(wraps_ahead)
    def _():
        straight_last(nb - 1, True)

    passed_last(nb - 1)

    @pl.when(jnp.logical_not(wraps_ahead))
    def _():
        straight_last(nb - 1, True)

    near = pl.ds(pl.multiple_of(odd * half, half), half)
    away = pl.ds(pl.multiple_of((1 - odd) * half, half), half)

    @pl.when(b >= relayed)
    def _():
        for role in (0, 2, 1, 3):
            for k in range(1 if role == 0 else 0, nb):
                from_final(role, lax.rem(b + k, nb)).wait_recv()
        home = zsend[b, 0] + sum(final[0, lax.rem(b + k, nb)] for k in range(1, nb))
        out_ref[0, :, near, :] = (home + sum(final[2, k] for k in range(nb))) * (1.0 / 12.0)
        out_ref[0, :, away, :] = sum(final[1, k] + final[3, k] for k in range(nb)) * (1.0 / 12.0)

    @pl.when(b < relayed)
    def _():
        for role in (2, 1, 3):
            from_final(role, b).wait_recv()
        out_ref[0, :, near, :] = (zsend[b, 0] + final[2, b]) * (1.0 / 12.0)
        out_ref[0, :, away, :] = (final[1, b] + final[3, b]) * (1.0 / 12.0)

    for k in range(1, nb):
        to_peer(k).wait_send()
    for j in range(nb):
        to_mate(j, 0).wait_send()
        to_mate(j, 1).wait_send()
        to_outer(j, own).wait_send()
        to_inner(j).wait_send()
    for j in mixed:
        @pl.when(jnp.logical_not(wraps))
        def _():
            to_outer_mixed(j).wait_send()

        @pl.when(wraps_ahead)
        def _():
            to_inner_mixed(j).wait_send()

    for j in range(nb):
        if j < relayed:
            @pl.when(b != j)
            def _():
                to_inbox(j).wait_send()

            @pl.when(b == j)
            def _():
                for role in (1, 2, 3):
                    to_final(j, role).wait_send()
        else:
            for role in (1, 2, 3):
                to_final(j, role).wait_send()

            @pl.when(b != j)
            def _():
                to_final(j, 0).wait_send()


def solution(mesh):
    nb = mesh.shape["band"]
    ng = mesh.shape["grid"]

    def per_device(orbitals, occupations):
        bands, _, depth, nx, ny = orbitals.shape
        rows = nx // nb
        half = rows // 2
        if depth != 2 or nb % 2 or nb < 4 or ng % 2 or ng < 6 or half % TILE:
            raise ValueError("unsupported sizes")
        f32, bf16 = jnp.float32, jnp.bfloat16
        dma = pltpu.SemaphoreType.DMA
        return pl.pallas_call(
            functools.partial(kernel, nb, ng),
            out_shape=jax.ShapeDtypeStruct((3, depth, rows, ny), f32),
            in_specs=[
                pl.BlockSpec(memory_space=pltpu.HBM),
                pl.BlockSpec(memory_space=pltpu.HBM),
            ],
            out_specs=pl.BlockSpec(memory_space=pltpu.VMEM),
            scratch_shapes=[
                pltpu.SMEM((bands,), f32),
                pltpu.VMEM((bands, 2, depth, nx, ny), bf16),
                pltpu.VMEM((nb, bands, 2, depth, half, ny), bf16),
                pltpu.VMEM((nb, bands - bands // 2 + 1, 2, depth, half, ny), bf16),
                pltpu.VMEM((nb, bands // 2, 2, depth, half, ny), bf16),
                pltpu.VMEM((nx, nx), bf16),
                pltpu.VMEM((ny, ny), bf16),
                pltpu.VMEM((2, depth, nx, ny), f32),
                pltpu.VMEM((nb - 1, 2, depth, rows, ny), f32),
                pltpu.VMEM((nb, 4, depth, half, ny), f32),
                pltpu.VMEM((nb - 1, 4, depth, half, ny), f32),
                pltpu.VMEM((4, nb, depth, half, ny), f32),
                dma,
                dma,
                dma((2, nb)),
                dma((2, nb)),
                dma((2, nb)),
                dma((2, nb)),
                dma((2, nb)),
                dma((2, nb)),
                dma((nb - 1,)),
                dma((nb - 1,)),
                dma((nb - 1,)),
                dma((nb - 1,)),
                dma((nb, 4)),
                dma((4, nb)),
                pltpu.SemaphoreType.REGULAR,
                pltpu.SemaphoreType.REGULAR,
            ],
            compiler_params=pltpu.CompilerParams(collective_id=0, has_side_effects=True, vmem_limit_bytes=55000 * 1024),
            name="current",
        )(pltpu.with_memory_space_constraint(occupations, pltpu.HBM), orbitals)

    return jax.shard_map(
        per_device,
        mesh=mesh,
        in_specs=(P("band", None, "grid", None, None), P("band")),
        out_specs=P(None, "grid", "band", None),
        check_vma=False,
    )
```

```python
import functools

import jax
import jax.numpy as jnp
from jax import lax
from jax.experimental import pallas as pl
from jax.experimental.pallas import tpu as pltpu
from jax.sharding import PartitionSpec as P

TILE = 16
MIXED = (0,)
HELD = 1


def stencil(n, flipped):
    row = lax.broadcasted_iota(jnp.int32, (n, n), 0)
    col = lax.broadcasted_iota(jnp.int32, (n, n), 1)
    d = col - row if flipped else row - col
    value = jnp.zeros((n, n), jnp.float32)
    for step, weight in ((1, 8.0), (-1, -8.0), (2, -1.0), (-2, 1.0)):
        hit = (d == step) | (d == step - n) | (d == step + n)
        value = jnp.where(hit, weight, value)
    return value.astype(jnp.bfloat16)


def kernel(
    nb, ng, occ_hbm, orb_ref, out_ref,
    occ_ref, own, mate, outer, inner, mx, my, plane_sum, plane_recv, zsend, inbox, final,
    occ_sem, own_sem, mate_send, mate_recv, outer_send, outer_recv, inner_send, inner_recv,
    plane_send_sem, plane_recv_sem, inbox_send, inbox_recv, final_send, final_recv, partner_in, next_in, wrap_in, peers_in,
):
    bands, _, depth, nx, ny = orb_ref.shape
    b = lax.axis_index("band")
    g = lax.axis_index("grid")
    odd = lax.rem(g, 2)
    turn = 1 - 2 * odd
    partner = g + turn
    ahead = lax.rem(g + 2 * turn + ng, ng)
    behind = lax.rem(g - 2 * turn + ng, ng)
    side = lax.rem(g - turn + ng, ng)
    layers = ng // 2
    layer = g // 2
    rows = nx // nb
    half = rows // 2
    split = bands // 2
    relayed = nb // 2

    load = pltpu.make_async_copy(orb_ref, own, own_sem)
    load.start()
    weights = pltpu.make_async_copy(occ_hbm, occ_ref, occ_sem)
    weights.start()

    barrier = pltpu.get_barrier_semaphore()
    last = layers - 1

    def tell(semaphore, band, grid):
        pl.semaphore_signal(semaphore, inc=1, device_id={"band": band, "grid": grid})

    @pl.when(odd == 0)
    def _():
        tell(barrier, b, partner)

    @pl.when(layer < last)
    def _():
        tell(barrier, b, g + 2)

    @pl.when(layer == 0)
    def _():
        tell(barrier, b, g + 2 * last)

    chip = b // 2
    tell(barrier, b + 1 - 2 * lax.rem(b, 2), g)
    for k in range(2, nb):
        @pl.when(2 * chip + k < nb)
        def _():
            tell(barrier, 2 * chip + k, g)

    earlier = odd + (layer > 0).astype(jnp.int32) + (layer == last).astype(jnp.int32) + 2 * chip + 1
    pl.semaphore_wait(barrier, earlier)

    @pl.when(odd == 1)
    def _():
        tell(partner_in, b, partner)

    @pl.when(layer > 0)
    def _():
        tell(next_in, b, g - 2)

    @pl.when(layer == last)
    def _():
        tell(wrap_in, b, g - 2 * last)

    for k in range(1, nb - 1):
        @pl.when(2 * chip - k >= 0)
        def _():
            tell(peers_in, 2 * chip - k, g)

    def rows_of(j, parity):
        return pl.ds(pl.multiple_of(j * rows + parity * half, half), half)

    passed, straight = pl.ds(0, split), pl.ds(split, bands - split)
    mixed = [j for j in MIXED if j < nb]
    last_passed = [split - (j in mixed) for j in range(nb)]

    def to_mate(j, kind, source=None):
        source = own if source is None else source
        part = (passed, straight)[kind]
        return pltpu.make_async_remote_copy(
            src_ref=source.at[part, :, :, rows_of(j, 1 - odd), :],
            dst_ref=mate.at[j, part],
            send_sem=mate_send.at[kind, j],
            recv_sem=mate_recv.at[kind, j],
            device_id={"band": b, "grid": partner},
        )

    def to_outer(j, start, source=None):
        source = own if source is None else source
        part = pl.ds(start, bands - start)
        return pltpu.make_async_remote_copy(
            src_ref=source.at[part, :, :, rows_of(j, odd), :],
            dst_ref=outer.at[j, pl.ds(start - split + 1, bands - start)],
            send_sem=outer_send.at[j],
            recv_sem=outer_recv.at[j],
            device_id={"band": b, "grid": behind},
        )

    def to_inner(j, stop):
        return pltpu.make_async_remote_copy(
            src_ref=mate.at[j, pl.ds(0, stop)],
            dst_ref=inner.at[j, pl.ds(0, stop)],
            send_sem=inner_send.at[j],
            recv_sem=inner_recv.at[j],
            device_id={"band": b, "grid": ahead},
        )

    def by_wrap(wrapping, j, act):
        if j not in mixed:
            act(split)
            return

        @pl.when(wrapping)
        def _():
            act(split)

        @pl.when(jnp.logical_not(wrapping))
        def _():
            act(split - 1)

    wraps = ((odd == 0) & (layer == 0)) | ((odd == 1) & (layer == layers - 1))
    wraps_ahead = ((odd == 0) & (layer == layers - 1)) | ((odd == 1) & (layer == 0))
    plain_behind = wraps
    plain_ahead = wraps_ahead
    def start_mate(skip):
        for kind in (0, 1):
            for j in range(nb):
                if kind or j >= skip:
                    to_mate(j, kind).start()

    def start_outer(skip):
        for j in range(skip, nb - HELD):
            by_wrap(plain_behind, j, lambda start: to_outer(j, start).start())

        @pl.when(jnp.logical_not(wraps_ahead))
        def _():
            for j in range(nb - HELD, nb):
                by_wrap(plain_behind, j, lambda start: to_outer(j, start).start())

    known = ((odd == 0) & (layer > 0)) | ((odd == 1) & (layer == last))

    @pl.when(odd == 1)
    def _():
        to_mate(0, 0, orb_ref).start()

    @pl.when(known)
    def _():
        by_wrap(plain_behind, 0, lambda start: to_outer(0, start, orb_ref).start())

    load.wait()

    @pl.when(known)
    def _():
        start_outer(1)

    @pl.when(2 * chip + 2 < nb)
    def _():
        pl.semaphore_wait(peers_in, nb - 2 * chip - 2)

    @pl.when(odd == 1)
    def _():
        start_mate(1)

    @pl.when(odd == 0)
    def _():
        pl.semaphore_wait(partner_in, 1)
        start_mate(0)

    @pl.when(layer < last)
    def _():
        pl.semaphore_wait(next_in, 1)

    @pl.when((odd == 1) & (layer < last))
    def _():
        start_outer(0)

    @pl.when(layer == 0)
    def _():
        pl.semaphore_wait(wrap_in, 1)

    @pl.when((odd == 0) & (layer == 0))
    def _():
        start_outer(0)

    mx[...] = stencil(nx, True)
    my[...] = stencil(ny, False)
    plane_sum[...] = jnp.zeros_like(plane_sum)
    zsend[...] = jnp.zeros_like(zsend)
    weights.wait()

    def lateral(n, carry):
        w = occ_ref[n]
        for s in range(depth):
            re = own[n, 0, s]
            im = own[n, 1, s]
            tx = jnp.dot(mx[...], jnp.concatenate([re, im], 1), preferred_element_type=jnp.float32)
            ty = jnp.dot(jnp.concatenate([re, im], 0), my[...], preferred_element_type=jnp.float32)
            wre = re.astype(jnp.float32) * w
            wim = im.astype(jnp.float32) * w
            plane_sum[0, s] += wre * tx[:, ny:] - wim * tx[:, :ny]
            plane_sum[1, s] += wre * ty[nx:] - wim * ty[:nx]
        return carry

    lax.fori_loop(0, bands, lateral, 0)

    def to_peer(k):
        peer = lax.rem(b + k, nb)
        return pltpu.make_async_remote_copy(
            src_ref=plane_sum.at[:, :, pl.ds(pl.multiple_of(peer * rows, rows), rows), :],
            dst_ref=plane_recv.at[k - 1],
            send_sem=plane_send_sem.at[k - 1],
            recv_sem=plane_recv_sem.at[k - 1],
            device_id={"band": peer, "grid": g},
        )

    for k in range(1, nb):
        to_peer(k).start()

    for j in range(nb):
        to_mate(j, 0).wait_recv()
        by_wrap(plain_ahead, j, lambda stop: to_inner(j, stop).start())

    @pl.when(wraps_ahead)
    def _():
        for j in range(nb - HELD, nb):
            by_wrap(plain_behind, j, lambda start: to_outer(j, start).start())

    mine = pl.ds(pl.multiple_of(b * rows, rows), rows)
    summed = plane_sum[:, :, mine, :]
    for k in range(1, nb):
        to_peer(k).wait_recv()
        summed = summed + plane_recv[k - 1]
    out_ref[1:3] = summed * (1.0 / 12.0)

    first = odd
    second = 1 - odd
    sign = turn.astype(jnp.float32)
    zero = jnp.zeros((half, ny), jnp.float32)

    def fields_of(held, n):
        return [tuple(held(n, q, p) for q in (0, 1)) for p in (first, second)]

    def bonds(n, low, high, sums):
        w = occ_ref[n] * sign
        low = [(re * w, im * w) for re, im in low]
        pairs = ((1, 0), (0, 0), (1, 1))
        return tuple(
            total + (low[i][0] * high[k][1] - low[i][1] * high[k][0]) for total, (i, k) in zip(sums, pairs)
        )

    def at_home(j):
        return lambda n, q, p: own[n, q, p, rows_of(j, odd), :].astype(jnp.float32)

    def at_mate(j):
        return lambda n, q, p: mate[j, n, q, p].astype(jnp.float32)

    def core_part(j):
        def step(n, sums):
            low, high = fields_of(at_home(j), n), fields_of(at_mate(j), n)
            w = occ_ref[n] * sign
            inside = tuple(
                total + (slab[0][0] * w * slab[1][1] - slab[0][1] * w * slab[1][0])
                for total, slab in zip(sums[3:], (low, high))
            )
            return bonds(n, low, high, sums[:3]) + inside

        n12, f02, f13, n01, n23 = lax.fori_loop(0, bands, step, (zero,) * 5, unroll=4)
        zsend[j, 0, first] += 8.0 * n01 - f02
        zsend[j, 0, second] += 8.0 * (n01 + n12) - f13
        zsend[j, 2, first] += 8.0 * (n12 + n23) - f02
        zsend[j, 2, second] += 8.0 * n23 - f13

    def straight_part(j):
        def step(n, sums):
            far = fields_of(lambda n, q, p: outer[j, n - split + 1, q, p].astype(jnp.float32), n)
            return bonds(n, fields_of(at_mate(j), n), far, sums)

        sums = lax.fori_loop(split, bands, step, (zero,) * 3, unroll=True)
        if j in mixed:
            sums = lax.fori_loop(split - jnp.where(plain_ahead, 0, 1), split, step, sums)
        n34, f24, f35 = sums
        zsend[j, 2, first] += -f24
        zsend[j, 2, second] += 8.0 * n34 - f35
        zsend[j, 3, first] = 8.0 * n34 - f24
        zsend[j, 3, second] = -f35

    def passed_part(j):
        def step(n, sums):
            far = fields_of(lambda n, q, p: inner[j, n, q, p].astype(jnp.float32), n)
            return bonds(n, far, fields_of(at_home(j), n), sums)

        sums = lax.fori_loop(0, last_passed[j], step, (zero,) * 3, unroll=True)
        if j in mixed:
            sums = lax.fori_loop(split - jnp.where(plain_behind, 1, 0), split, step, sums)
        n10, f20, f11 = sums
        zsend[j, 0, first] += 8.0 * n10 - f20
        zsend[j, 0, second] += -f11
        zsend[j, 1, first] = -f20
        zsend[j, 1, second] = 8.0 * n10 - f11

    def to_inbox(j, kind):
        slot = lax.rem(b - j - 1 + nb, nb)
        return pltpu.make_async_remote_copy(
            src_ref=zsend.at[j, pl.ds(2 * kind, 2)],
            dst_ref=inbox.at[slot, pl.ds(2 * kind, 2)],
            send_sem=inbox_send.at[kind, j],
            recv_sem=inbox_recv.at[kind, slot],
            device_id={"band": j, "grid": g},
        )

    def from_inbox(slot, kind):
        return pltpu.make_async_remote_copy(
            src_ref=zsend.at[0, pl.ds(2 * kind, 2)],
            dst_ref=inbox.at[slot, pl.ds(2 * kind, 2)],
            send_sem=inbox_send.at[kind, 0],
            recv_sem=inbox_recv.at[kind, slot],
            device_id={"band": b, "grid": partner},
        )

    def to_final(j, role):
        return pltpu.make_async_remote_copy(
            src_ref=zsend.at[j, role],
            dst_ref=final.at[role, b],
            send_sem=final_send.at[j, role],
            recv_sem=final_recv.at[role, b],
            device_id={"band": j, "grid": (g, side, partner, ahead)[role]},
        )

    def from_final(role, source):
        return pltpu.make_async_remote_copy(
            src_ref=zsend.at[0, 0],
            dst_ref=final.at[role, source],
            send_sem=final_send.at[0, 0],
            recv_sem=final_recv.at[role, source],
            device_id={"band": b, "grid": partner},
        )

    def arrive_mate(j):
        to_mate(j, 1).wait_recv()

    def arrive_outer(j):
        by_wrap(plain_ahead, j, lambda start: to_outer(j, start).wait_recv())

    def arrive_inner(j):
        by_wrap(plain_behind, j, lambda stop: to_inner(j, stop).wait_recv())

    def finish(j):
        @pl.when(b == j)
        def _():
            for kind, roles in ((1, (3, 2)), (0, (1,))):
                pair = pl.ds(2 * kind, 2)
                for slot in range(nb - 1):
                    from_inbox(slot, kind).wait_recv()
                zsend[j, pair] = zsend[j, pair] + sum(inbox[slot, pair] for slot in range(nb - 1))
                for role in roles:
                    to_final(j, role).start()

    for j in range(relayed):
        arrive_mate(j)
        core_part(j)
        arrive_outer(j)
        straight_part(j)

        @pl.when(b != j)
        def _():
            to_inbox(j, 1).start()

        arrive_inner(j)
        passed_part(j)

        @pl.when(b != j)
        def _():
            to_inbox(j, 0).start()

        if j:
            finish(j - 1)

    def send_own(j):
        @pl.when(b != j)
        def _():
            to_final(j, 0).start()

    for j in range(relayed, nb - 1):
        arrive_mate(j)
        if j > relayed:
            to_final(j - 1, 2).start()
        core_part(j)
        arrive_outer(j)
        straight_part(j)
        to_final(j, 3).start()
        arrive_inner(j)
        passed_part(j)
        to_final(j, 1).start()
        send_own(j)

    end = nb - 1

    @pl.when(wraps)
    def _():
        arrive_inner(end)
        passed_part(end)
        to_final(end, 1).start()

    finish(relayed - 1)
    arrive_mate(end)
    to_final(end - 1, 2).start()

    @pl.when(wraps_ahead)
    def _():
        arrive_outer(end)
        straight_part(end)
        to_final(end, 3).start()

    core_part(end)

    @pl.when(wraps)
    def _():
        send_own(end)

    @pl.when(wraps_ahead)
    def _():
        to_final(end, 2).start()

    @pl.when(jnp.logical_not(wraps))
    def _():
        arrive_inner(end)
        passed_part(end)
        to_final(end, 1).start()
        send_own(end)

    @pl.when(jnp.logical_not(wraps_ahead))
    def _():
        arrive_outer(end)
        straight_part(end)
        to_final(end, 3).start()
        to_final(end, 2).start()

    near = pl.ds(pl.multiple_of(odd * half, half), half)
    away = pl.ds(pl.multiple_of((1 - odd) * half, half), half)

    @pl.when(b >= relayed)
    def _():
        for role in (0, 2, 3, 1):
            for k in range(1 if role == 0 else 0, nb):
                from_final(role, lax.rem(b + k, nb)).wait_recv()
        home = zsend[b, 0] + sum(final[0, lax.rem(b + k, nb)] for k in range(1, nb))
        out_ref[0, :, near, :] = (home + sum(final[3, k] for k in range(nb))) * (1.0 / 12.0)
        out_ref[0, :, away, :] = sum(final[2, k] + final[1, k] for k in range(nb)) * (1.0 / 12.0)

    @pl.when(b < relayed)
    def _():
        for role in (2, 3, 1):
            from_final(role, b).wait_recv()
        out_ref[0, :, near, :] = (zsend[b, 0] + final[3, b]) * (1.0 / 12.0)
        out_ref[0, :, away, :] = (final[2, b] + final[1, b]) * (1.0 / 12.0)

    for k in range(1, nb):
        to_peer(k).wait_send()
    for j in range(nb):
        to_mate(j, 0).wait_send()
        to_mate(j, 1).wait_send()
        by_wrap(plain_behind, j, lambda start: to_outer(j, start).wait_send())
        by_wrap(plain_ahead, j, lambda stop: to_inner(j, stop).wait_send())
    for j in range(nb):
        if j < relayed:
            @pl.when(b != j)
            def _():
                to_inbox(j, 0).wait_send()
                to_inbox(j, 1).wait_send()

            @pl.when(b == j)
            def _():
                for role in (1, 2, 3):
                    to_final(j, role).wait_send()
        else:
            for role in (1, 2, 3):
                to_final(j, role).wait_send()

            @pl.when(b != j)
            def _():
                to_final(j, 0).wait_send()


def solution(mesh):
    nb = mesh.shape["band"]
    ng = mesh.shape["grid"]

    def per_device(orbitals, occupations):
        bands, _, depth, nx, ny = orbitals.shape
        rows = nx // nb
        half = rows // 2
        if depth != 2 or nb % 2 or nb < 4 or ng % 2 or ng < 6 or half % TILE:
            raise ValueError("unsupported sizes")
        f32, bf16 = jnp.float32, jnp.bfloat16
        dma = pltpu.SemaphoreType.DMA
        return pl.pallas_call(
            functools.partial(kernel, nb, ng),
            out_shape=jax.ShapeDtypeStruct((3, depth, rows, ny), f32),
            in_specs=[
                pl.BlockSpec(memory_space=pltpu.HBM),
                pl.BlockSpec(memory_space=pltpu.HBM),
            ],
            out_specs=pl.BlockSpec(memory_space=pltpu.VMEM),
            scratch_shapes=[
                pltpu.SMEM((bands,), f32),
                pltpu.VMEM((bands, 2, depth, nx, ny), bf16),
                pltpu.VMEM((nb, bands, 2, depth, half, ny), bf16),
                pltpu.VMEM((nb, bands - bands // 2 + 1, 2, depth, half, ny), bf16),
                pltpu.VMEM((nb, bands // 2, 2, depth, half, ny), bf16),
                pltpu.VMEM((nx, nx), bf16),
                pltpu.VMEM((ny, ny), bf16),
                pltpu.VMEM((2, depth, nx, ny), f32),
                pltpu.VMEM((nb - 1, 2, depth, rows, ny), f32),
                pltpu.VMEM((nb, 4, depth, half, ny), f32),
                pltpu.VMEM((nb - 1, 4, depth, half, ny), f32),
                pltpu.VMEM((4, nb, depth, half, ny), f32),
                dma,
                dma,
                dma((2, nb)),
                dma((2, nb)),
                dma((nb,)),
                dma((nb,)),
                dma((nb,)),
                dma((nb,)),
                dma((nb - 1,)),
                dma((nb - 1,)),
                dma((2, nb - 1)),
                dma((2, nb - 1)),
                dma((nb, 4)),
                dma((4, nb)),
                pltpu.SemaphoreType.REGULAR,
                pltpu.SemaphoreType.REGULAR,
                pltpu.SemaphoreType.REGULAR,
                pltpu.SemaphoreType.REGULAR,
            ],
            compiler_params=pltpu.CompilerParams(collective_id=0, has_side_effects=True, vmem_limit_bytes=55000 * 1024),
            name="current",
        )(pltpu.with_memory_space_constraint(occupations, pltpu.HBM), orbitals)

    return jax.shard_map(
        per_device,
        mesh=mesh,
        in_specs=(P("band", None, "grid", None, None), P("band")),
        out_specs=P(None, "grid", "band", None),
        check_vma=False,
    )
```

```python
import functools

import jax
import jax.numpy as jnp
from jax import lax
from jax.experimental import pallas as pl
from jax.experimental.pallas import tpu as pltpu
from jax.sharding import PartitionSpec as P

TILE = 16
MIXED = 1
HELD = 1


def stencil(n, flipped):
    row = lax.broadcasted_iota(jnp.int32, (n, n), 0)
    col = lax.broadcasted_iota(jnp.int32, (n, n), 1)
    d = col - row if flipped else row - col
    value = jnp.zeros((n, n), jnp.float32)
    for step, weight in ((1, 8.0), (-1, -8.0), (2, -1.0), (-2, 1.0)):
        hit = (d == step) | (d == step - n) | (d == step + n)
        value = jnp.where(hit, weight, value)
    return value.astype(jnp.bfloat16)


def kernel(
    nb, ng, occ_hbm, orb_ref, out_ref,
    occ_ref, own, mate, outer, inner, mx, my, plane_sum, plane_recv, zsend, inbox, final,
    occ_sem, own_sem, mate_send, mate_recv, outer_send, outer_recv, inner_send, inner_recv,
    plane_send_sem, plane_recv_sem, inbox_send, inbox_recv, final_send, final_recv, partner_in, next_in, wrap_in, peers_in,
):
    bands, _, depth, nx, ny = orb_ref.shape
    b = lax.axis_index("band")
    g = lax.axis_index("grid")
    odd = lax.rem(g, 2)
    turn = 1 - 2 * odd
    partner = g + turn
    ahead = lax.rem(g + 2 * turn + ng, ng)
    behind = lax.rem(g - 2 * turn + ng, ng)
    side = lax.rem(g - turn + ng, ng)
    layers = ng // 2
    layer = g // 2
    rows = nx // nb
    half = rows // 2
    split = bands // 2
    relayed = nb // 2

    load = pltpu.make_async_copy(orb_ref, own, own_sem)
    load.start()
    weights = pltpu.make_async_copy(occ_hbm, occ_ref, occ_sem)
    weights.start()

    barrier = pltpu.get_barrier_semaphore()
    last = layers - 1

    def tell(semaphore, band, grid):
        pl.semaphore_signal(semaphore, inc=1, device_id={"band": band, "grid": grid})

    @pl.when(odd == 0)
    def _():
        tell(barrier, b, partner)

    @pl.when(layer < last)
    def _():
        tell(barrier, b, g + 2)

    @pl.when(layer == 0)
    def _():
        tell(barrier, b, g + 2 * last)

    chip = b // 2
    tell(barrier, b + 1 - 2 * lax.rem(b, 2), g)
    for k in range(2, nb):
        @pl.when(2 * chip + k < nb)
        def _():
            tell(barrier, 2 * chip + k, g)

    earlier = odd + (layer > 0).astype(jnp.int32) + (layer == last).astype(jnp.int32) + 2 * chip + 1
    pl.semaphore_wait(barrier, earlier)

    @pl.when(odd == 1)
    def _():
        tell(partner_in, b, partner)

    @pl.when(layer > 0)
    def _():
        tell(next_in, b, g - 2)

    @pl.when(layer == last)
    def _():
        tell(wrap_in, b, g - 2 * last)

    for k in range(1, nb - 1):
        @pl.when(2 * chip - k >= 0)
        def _():
            tell(peers_in, 2 * chip - k, g)

    def bytes_of(ref, semaphore):
        return pltpu.make_async_remote_copy(
            src_ref=ref, dst_ref=ref, send_sem=semaphore, recv_sem=semaphore, device_id={"band": b, "grid": partner}
        )

    def rows_of(j, parity):
        return pl.ds(pl.multiple_of(j * rows + parity * half, half), half)

    passed, straight = pl.ds(0, split), pl.ds(split, bands - split)
    mixed = range(MIXED)
    last_passed = [split - (j in mixed) for j in range(nb)]

    def to_mate(j, kind, source=None):
        source = own if source is None else source
        part = (passed, straight)[kind]
        return pltpu.make_async_remote_copy(
            src_ref=source.at[part, :, :, rows_of(j, 1 - odd), :],
            dst_ref=mate.at[j, part],
            send_sem=mate_send,
            recv_sem=mate_recv.at[kind, j],
            device_id={"band": b, "grid": partner},
        )

    def to_outer(j, start, source=None):
        source = own if source is None else source
        part = pl.ds(start, bands - start)
        return pltpu.make_async_remote_copy(
            src_ref=source.at[part, :, :, rows_of(j, odd), :],
            dst_ref=outer.at[j, pl.ds(start - split + 1, bands - start)],
            send_sem=outer_send.at[int(j in mixed)],
            recv_sem=outer_recv.at[j],
            device_id={"band": b, "grid": behind},
        )

    def to_inner(j, stop):
        return pltpu.make_async_remote_copy(
            src_ref=mate.at[j, pl.ds(0, stop)],
            dst_ref=inner.at[j, pl.ds(0, stop)],
            send_sem=inner_send.at[int(j in mixed)],
            recv_sem=inner_recv.at[j],
            device_id={"band": b, "grid": ahead},
        )

    def by_wrap(wrapping, j, act):
        if j not in mixed:
            act(split)
            return

        @pl.when(wrapping)
        def _():
            act(split)

        @pl.when(jnp.logical_not(wrapping))
        def _():
            act(split - 1)

    wraps = ((odd == 0) & (layer == 0)) | ((odd == 1) & (layer == layers - 1))
    wraps_ahead = ((odd == 0) & (layer == layers - 1)) | ((odd == 1) & (layer == 0))
    plain_behind = wraps
    plain_ahead = wraps_ahead
    def start_mate(skip):
        for kind in (0, 1):
            for j in range(nb):
                if kind or j >= skip:
                    to_mate(j, kind).start()

    def start_outer(skip):
        for j in range(skip, nb - HELD):
            by_wrap(plain_behind, j, lambda start: to_outer(j, start).start())

        @pl.when(jnp.logical_not(wraps_ahead))
        def _():
            for j in range(nb - HELD, nb):
                by_wrap(plain_behind, j, lambda start: to_outer(j, start).start())

    known = ((odd == 0) & (layer > 0)) | ((odd == 1) & (layer == last))

    @pl.when(odd == 1)
    def _():
        to_mate(0, 0, orb_ref).start()

    @pl.when(known)
    def _():
        by_wrap(plain_behind, 0, lambda start: to_outer(0, start, orb_ref).start())

    load.wait()

    @pl.when(known)
    def _():
        start_outer(1)

    @pl.when(2 * chip + 2 < nb)
    def _():
        pl.semaphore_wait(peers_in, nb - 2 * chip - 2)

    @pl.when(odd == 1)
    def _():
        start_mate(1)

    @pl.when(odd == 0)
    def _():
        pl.semaphore_wait(partner_in, 1)
        start_mate(0)

    @pl.when(layer < last)
    def _():
        pl.semaphore_wait(next_in, 1)

    @pl.when((odd == 1) & (layer < last))
    def _():
        start_outer(0)

    @pl.when(layer == 0)
    def _():
        pl.semaphore_wait(wrap_in, 1)

    @pl.when((odd == 0) & (layer == 0))
    def _():
        start_outer(0)

    mx[...] = stencil(nx, True)
    my[...] = stencil(ny, False)
    plane_sum[...] = jnp.zeros_like(plane_sum)
    zsend[...] = jnp.zeros_like(zsend)
    weights.wait()

    def lateral(n, carry):
        w = occ_ref[n]
        for s in range(depth):
            re = own[n, 0, s]
            im = own[n, 1, s]
            tx = jnp.dot(mx[...], jnp.concatenate([re, im], 1), preferred_element_type=jnp.float32)
            ty = jnp.dot(jnp.concatenate([re, im], 0), my[...], preferred_element_type=jnp.float32)
            wre = re.astype(jnp.float32) * w
            wim = im.astype(jnp.float32) * w
            plane_sum[0, s] += wre * tx[:, ny:] - wim * tx[:, :ny]
            plane_sum[1, s] += wre * ty[nx:] - wim * ty[:nx]
        return carry

    lax.fori_loop(0, bands, lateral, 0)

    def to_peer(k):
        peer = lax.rem(b + k, nb)
        return pltpu.make_async_remote_copy(
            src_ref=plane_sum.at[:, :, pl.ds(pl.multiple_of(peer * rows, rows), rows), :],
            dst_ref=plane_recv.at[k - 1],
            send_sem=plane_send_sem,
            recv_sem=plane_recv_sem,
            device_id={"band": peer, "grid": g},
        )

    for k in range(1, nb):
        to_peer(k).start()

    for j in range(nb):
        to_mate(j, 0).wait_recv()
        by_wrap(plain_ahead, j, lambda stop: to_inner(j, stop).start())

    @pl.when(wraps_ahead)
    def _():
        for j in range(nb - HELD, nb):
            by_wrap(plain_behind, j, lambda start: to_outer(j, start).start())

    mine = pl.ds(pl.multiple_of(b * rows, rows), rows)
    summed = plane_sum[:, :, mine, :]
    bytes_of(plane_recv, plane_recv_sem).wait_recv()
    for k in range(1, nb):
        summed = summed + plane_recv[k - 1]
    out_ref[1:3] = summed * (1.0 / 12.0)

    first = odd
    second = 1 - odd
    sign = turn.astype(jnp.float32)
    zero = jnp.zeros((half, ny), jnp.float32)

    def fields_of(held, n):
        return [tuple(held(n, q, p) for q in (0, 1)) for p in (first, second)]

    def bonds(n, low, high, sums):
        w = occ_ref[n] * sign
        low = [(re * w, im * w) for re, im in low]
        pairs = ((1, 0), (0, 0), (1, 1))
        return tuple(
            total + (low[i][0] * high[k][1] - low[i][1] * high[k][0]) for total, (i, k) in zip(sums, pairs)
        )

    def at_home(j):
        return lambda n, q, p: own[n, q, p, rows_of(j, odd), :].astype(jnp.float32)

    def at_mate(j):
        return lambda n, q, p: mate[j, n, q, p].astype(jnp.float32)

    def core_part(j):
        def step(n, sums):
            low, high = fields_of(at_home(j), n), fields_of(at_mate(j), n)
            w = occ_ref[n] * sign
            inside = tuple(
                total + (slab[0][0] * w * slab[1][1] - slab[0][1] * w * slab[1][0])
                for total, slab in zip(sums[3:], (low, high))
            )
            return bonds(n, low, high, sums[:3]) + inside

        n12, f02, f13, n01, n23 = lax.fori_loop(0, bands, step, (zero,) * 5, unroll=4)
        zsend[j, 0, first] += 8.0 * n01 - f02
        zsend[j, 0, second] += 8.0 * (n01 + n12) - f13
        zsend[j, 2, first] += 8.0 * (n12 + n23) - f02
        zsend[j, 2, second] += 8.0 * n23 - f13

    def straight_part(j):
        def step(n, sums):
            far = fields_of(lambda n, q, p: outer[j, n - split + 1, q, p].astype(jnp.float32), n)
            return bonds(n, fields_of(at_mate(j), n), far, sums)

        sums = lax.fori_loop(split, bands, step, (zero,) * 3, unroll=True)
        if j in mixed:
            sums = lax.fori_loop(split - jnp.where(plain_ahead, 0, 1), split, step, sums)
        n34, f24, f35 = sums
        zsend[j, 2, first] += -f24
        zsend[j, 2, second] += 8.0 * n34 - f35
        zsend[j, 3, first] = 8.0 * n34 - f24
        zsend[j, 3, second] = -f35

    def passed_part(j):
        def step(n, sums):
            far = fields_of(lambda n, q, p: inner[j, n, q, p].astype(jnp.float32), n)
            return bonds(n, far, fields_of(at_home(j), n), sums)

        sums = lax.fori_loop(0, last_passed[j], step, (zero,) * 3, unroll=True)
        if j in mixed:
            sums = lax.fori_loop(split - jnp.where(plain_behind, 1, 0), split, step, sums)
        n10, f20, f11 = sums
        zsend[j, 0, first] += 8.0 * n10 - f20
        zsend[j, 0, second] += -f11
        zsend[j, 1, first] = -f20
        zsend[j, 1, second] = 8.0 * n10 - f11

    def to_inbox(j, role):
        slot = lax.rem(b - j - 1 + nb, nb)
        return pltpu.make_async_remote_copy(
            src_ref=zsend.at[j, role],
            dst_ref=inbox.at[role, slot],
            send_sem=inbox_send,
            recv_sem=inbox_recv.at[role % 2 + role // 3],
            device_id={"band": j, "grid": g},
        )

    def to_final(j, role):
        return pltpu.make_async_remote_copy(
            src_ref=zsend.at[j, role],
            dst_ref=final.at[role * nb + b],
            send_sem=final_send,
            recv_sem=final_recv,
            device_id={"band": j, "grid": (g, side, partner, ahead)[role]},
        )

    def arrive_mate(j):
        to_mate(j, 1).wait_recv()

    def arrive_outer(j):
        by_wrap(plain_ahead, j, lambda start: to_outer(j, start).wait_recv())

    def arrive_inner(j):
        by_wrap(plain_behind, j, lambda stop: to_inner(j, stop).wait_recv())

    def finish(j):
        @pl.when(b == j)
        def _():
            for part, roles in ((2, (3,)), (1, (1,)), (0, (0, 2))):
                bytes_of(inbox.at[pl.ds(0, len(roles))], inbox_recv.at[part]).wait_recv()
                for role in roles:
                    zsend[j, role] = zsend[j, role] + sum(inbox[role, slot] for slot in range(nb - 1))
                    if role:
                        to_final(j, role).start()

    for j in range(relayed):
        arrive_mate(j)
        core_part(j)
        arrive_outer(j)
        straight_part(j)

        @pl.when(b != j)
        def _():
            to_inbox(j, 3).start()

        arrive_inner(j)
        passed_part(j)

        @pl.when(b != j)
        def _():
            for role in (1, 2, 0):
                to_inbox(j, role).start()

        if j:
            finish(j - 1)

    def send_own(j):
        @pl.when(b != j)
        def _():
            to_final(j, 0).start()

    for j in range(relayed, nb - 1):
        arrive_mate(j)
        if j > relayed:
            to_final(j - 1, 2).start()
        core_part(j)
        arrive_outer(j)
        straight_part(j)
        to_final(j, 3).start()
        arrive_inner(j)
        passed_part(j)
        to_final(j, 1).start()
        send_own(j)

    end = nb - 1

    @pl.when(wraps)
    def _():
        arrive_inner(end)
        passed_part(end)
        to_final(end, 1).start()

    finish(relayed - 1)
    arrive_mate(end)
    to_final(end - 1, 2).start()

    @pl.when(wraps_ahead)
    def _():
        arrive_outer(end)
        straight_part(end)
        to_final(end, 3).start()

    core_part(end)

    @pl.when(wraps)
    def _():
        send_own(end)

    @pl.when(wraps_ahead)
    def _():
        to_final(end, 2).start()

    @pl.when(jnp.logical_not(wraps))
    def _():
        arrive_inner(end)
        passed_part(end)
        to_final(end, 1).start()
        send_own(end)

    @pl.when(jnp.logical_not(wraps_ahead))
    def _():
        arrive_outer(end)
        straight_part(end)
        to_final(end, 3).start()
        to_final(end, 2).start()

    near = pl.ds(pl.multiple_of(odd * half, half), half)
    away = pl.ds(pl.multiple_of((1 - odd) * half, half), half)

    @pl.when(b >= relayed)
    def _():
        bytes_of(final.at[pl.ds(0, 4 * nb - 1)], final_recv).wait_recv()
        home = zsend[b, 0] + sum(final[lax.rem(b + k, nb)] for k in range(1, nb))
        out_ref[0, :, near, :] = (home + sum(final[3 * nb + k] for k in range(nb))) * (1.0 / 12.0)
        out_ref[0, :, away, :] = sum(final[2 * nb + k] + final[nb + k] for k in range(nb)) * (1.0 / 12.0)

    @pl.when(b < relayed)
    def _():
        bytes_of(final.at[pl.ds(0, 3)], final_recv).wait_recv()
        out_ref[0, :, near, :] = (zsend[b, 0] + final[3 * nb + b]) * (1.0 / 12.0)
        out_ref[0, :, away, :] = (final[2 * nb + b] + final[nb + b]) * (1.0 / 12.0)

    bytes_of(plane_recv, plane_send_sem).wait_send()
    bytes_of(mate, mate_send).wait_send()
    bytes_of(outer.at[pl.ds(MIXED, nb - MIXED), pl.ds(1, bands - split)], outer_send.at[0]).wait_send()
    bytes_of(inner.at[pl.ds(MIXED, nb - MIXED)], inner_send.at[0]).wait_send()
    if MIXED:
        whole = pl.ds(0, MIXED)
        by_wrap(plain_behind, 0, lambda start: bytes_of(
            outer.at[whole, pl.ds(start - split + 1, bands - start)], outer_send.at[1]).wait_send())
        by_wrap(plain_ahead, 0, lambda stop: bytes_of(inner.at[whole, pl.ds(0, stop)], inner_send.at[1]).wait_send())
    direct = 4 * (nb - relayed)

    @pl.when(b >= relayed)
    def _():
        bytes_of(zsend.at[pl.ds(0, relayed)], inbox_send).wait_send()
        bytes_of(final.at[pl.ds(0, direct - 1)], final_send).wait_send()

    @pl.when(b < relayed)
    def _():
        bytes_of(zsend.at[pl.ds(0, relayed - 1)], inbox_send).wait_send()
        bytes_of(final.at[pl.ds(0, direct + 3)], final_send).wait_send()


def solution(mesh):
    nb = mesh.shape["band"]
    ng = mesh.shape["grid"]

    def per_device(orbitals, occupations):
        bands, _, depth, nx, ny = orbitals.shape
        rows = nx // nb
        half = rows // 2
        if depth != 2 or nb % 2 or nb < 4 or ng % 2 or ng < 6 or half % TILE:
            raise ValueError("unsupported sizes")
        f32, bf16 = jnp.float32, jnp.bfloat16
        dma = pltpu.SemaphoreType.DMA
        return pl.pallas_call(
            functools.partial(kernel, nb, ng),
            out_shape=jax.ShapeDtypeStruct((3, depth, rows, ny), f32),
            in_specs=[
                pl.BlockSpec(memory_space=pltpu.HBM),
                pl.BlockSpec(memory_space=pltpu.HBM),
            ],
            out_specs=pl.BlockSpec(memory_space=pltpu.VMEM),
            scratch_shapes=[
                pltpu.SMEM((bands,), f32),
                pltpu.VMEM((bands, 2, depth, nx, ny), bf16),
                pltpu.VMEM((nb, bands, 2, depth, half, ny), bf16),
                pltpu.VMEM((nb, bands - bands // 2 + 1, 2, depth, half, ny), bf16),
                pltpu.VMEM((nb, bands // 2, 2, depth, half, ny), bf16),
                pltpu.VMEM((nx, nx), bf16),
                pltpu.VMEM((ny, ny), bf16),
                pltpu.VMEM((2, depth, nx, ny), f32),
                pltpu.VMEM((nb - 1, 2, depth, rows, ny), f32),
                pltpu.VMEM((nb, 4, depth, half, ny), f32),
                pltpu.VMEM((4, nb - 1, depth, half, ny), f32),
                pltpu.VMEM((4 * nb, depth, half, ny), f32),
                dma,
                dma,
                dma,
                dma((2, nb)),
                dma((2,)),
                dma((nb,)),
                dma((2,)),
                dma((nb,)),
                dma,
                dma,
                dma,
                dma((3,)),
                dma,
                dma,
                pltpu.SemaphoreType.REGULAR,
                pltpu.SemaphoreType.REGULAR,
                pltpu.SemaphoreType.REGULAR,
                pltpu.SemaphoreType.REGULAR,
            ],
            compiler_params=pltpu.CompilerParams(collective_id=0, has_side_effects=True, vmem_limit_bytes=55000 * 1024),
            name="current",
        )(pltpu.with_memory_space_constraint(occupations, pltpu.HBM), orbitals)

    return jax.shard_map(
        per_device,
        mesh=mesh,
        in_specs=(P("band", None, "grid", None, None), P("band")),
        out_specs=P(None, "grid", "band", None),
        check_vma=False,
    )
```

```python
import functools

import jax
import jax.numpy as jnp
from jax import lax
from jax.experimental import pallas as pl
from jax.experimental.pallas import tpu as pltpu
from jax.sharding import PartitionSpec as P

TILE = 16
MIXED = (3, 1)
HELD = 1


def stencil(n, flipped):
    row = lax.broadcasted_iota(jnp.int32, (n, n), 0)
    col = lax.broadcasted_iota(jnp.int32, (n, n), 1)
    d = col - row if flipped else row - col
    value = jnp.zeros((n, n), jnp.float32)
    for step, weight in ((1, 8.0), (-1, -8.0), (2, -1.0), (-2, 1.0)):
        hit = (d == step) | (d == step - n) | (d == step + n)
        value = jnp.where(hit, weight, value)
    return value.astype(jnp.bfloat16)


def kernel(
    nb, ng, occ_hbm, orb_ref, out_ref,
    occ_ref, own, mate, outer, inner, mx, my, plane_sum, plane_recv, zsend, inbox, final, measure,
    occ_sem, own_sem, sent, mate_recv, outer_recv, inner_recv, plane_recv_sem, inbox_recv, final_recv, answers, wrap_in,
):
    bands, _, depth, nx, ny = orb_ref.shape
    b = lax.axis_index("band")
    g = lax.axis_index("grid")
    odd = lax.rem(g, 2)
    turn = 1 - 2 * odd
    partner = g + turn
    ahead = lax.rem(g + 2 * turn + ng, ng)
    behind = lax.rem(g - 2 * turn + ng, ng)
    side = lax.rem(g - turn + ng, ng)
    layers = ng // 2
    layer = g // 2
    rows = nx // nb
    half = rows // 2
    split = bands // 2
    relayed = nb // 2

    load = pltpu.make_async_copy(orb_ref, own, own_sem)
    load.start()
    weights = pltpu.make_async_copy(occ_hbm, occ_ref, occ_sem)
    weights.start()

    barrier = pltpu.get_barrier_semaphore()
    last = layers - 1

    def tell(semaphore, band, grid):
        pl.semaphore_signal(semaphore, inc=1, device_id={"band": band, "grid": grid})

    @pl.when(odd == 0)
    def _():
        tell(barrier, b, partner)

    @pl.when(layer < last)
    def _():
        tell(barrier, b, g + 2)

    @pl.when(layer == 0)
    def _():
        tell(barrier, b, g + 2 * last)

    chip = b // 2
    tell(barrier, b + 1 - 2 * lax.rem(b, 2), g)
    for k in range(2, nb):
        @pl.when(2 * chip + k < nb)
        def _():
            tell(barrier, 2 * chip + k, g)

    earlier = odd + (layer > 0).astype(jnp.int32) + (layer == last).astype(jnp.int32) + 2 * chip + 1
    pl.semaphore_wait(barrier, earlier)

    @pl.when(odd == 1)
    def _():
        tell(answers, b, partner)

    @pl.when(layer > 0)
    def _():
        tell(answers, b, g - 2)

    @pl.when(layer == last)
    def _():
        tell(wrap_in, b, g - 2 * last)

    for k in range(1, nb - 1):
        @pl.when(2 * chip - k >= 0)
        def _():
            tell(answers, 2 * chip - k, g)

    def bytes_of(ref, semaphore):
        return pltpu.make_async_remote_copy(
            src_ref=ref, dst_ref=ref, send_sem=semaphore, recv_sem=semaphore, device_id={"band": b, "grid": partner}
        )

    def rows_of(j, parity):
        return pl.ds(pl.multiple_of(j * rows + parity * half, half), half)

    passed, straight = pl.ds(0, split), pl.ds(split, bands - split)

    def to_mate(j, kind, source=None):
        source = own if source is None else source
        part = (passed, straight)[kind]
        return pltpu.make_async_remote_copy(
            src_ref=source.at[part, :, :, rows_of(j, 1 - odd), :],
            dst_ref=mate.at[j, part],
            send_sem=sent,
            recv_sem=mate_recv.at[kind, j],
            device_id={"band": b, "grid": partner},
        )

    def to_outer(j, start, source=None):
        source = own if source is None else source
        part = pl.ds(start, bands - start)
        return pltpu.make_async_remote_copy(
            src_ref=source.at[part, :, :, rows_of(j, odd), :],
            dst_ref=outer.at[j, pl.ds(start - split + 1, bands - start)],
            send_sem=sent,
            recv_sem=outer_recv.at[j],
            device_id={"band": b, "grid": behind},
        )

    def to_inner(j, stop):
        return pltpu.make_async_remote_copy(
            src_ref=mate.at[j, pl.ds(0, stop)],
            dst_ref=inner.at[j, pl.ds(0, stop)],
            send_sem=sent,
            recv_sem=inner_recv.at[j],
            device_id={"band": b, "grid": ahead},
        )

    def by_wrap(wrapping, j, act):
        if j >= max(MIXED):
            act(split)
            return
        plain = wrapping
        for parity in (0, 1):
            if j >= MIXED[parity]:
                plain = plain | (odd == parity)

        @pl.when(plain)
        def _():
            act(split)

        @pl.when(jnp.logical_not(plain))
        def _():
            act(split - 1)

    def shifted(wrapping, j):
        by_parity = jnp.where(odd == 1, int(j < MIXED[1]), int(j < MIXED[0]))
        return jnp.where(wrapping, 0, by_parity)

    wraps = ((odd == 0) & (layer == 0)) | ((odd == 1) & (layer == layers - 1))
    wraps_ahead = ((odd == 0) & (layer == layers - 1)) | ((odd == 1) & (layer == 0))
    def start_mate(skip):
        for kind in (0, 1):
            for j in range(nb):
                if kind or j >= skip:
                    to_mate(j, kind).start()

    def start_outer(skip):
        for j in range(skip, nb - HELD):
            by_wrap(wraps, j, lambda start: to_outer(j, start).start())

        @pl.when(jnp.logical_not(wraps_ahead))
        def _():
            for j in range(nb - HELD, nb):
                by_wrap(wraps, j, lambda start: to_outer(j, start).start())

    known = ((odd == 0) & (layer > 0)) | ((odd == 1) & (layer == last))

    @pl.when(odd == 1)
    def _():
        to_mate(0, 0, orb_ref).start()

    @pl.when(known)
    def _():
        by_wrap(wraps, 0, lambda start: to_outer(0, start, orb_ref).start())

    load.wait()

    @pl.when(known)
    def _():
        start_outer(1)

    later = nb - 2 * chip - 2 + (1 - odd) + (layer < last).astype(jnp.int32)

    @pl.when(later > 0)
    def _():
        pl.semaphore_wait(answers, later)

    @pl.when(odd == 1)
    def _():
        start_mate(1)

    @pl.when(odd == 0)
    def _():
        start_mate(0)

    @pl.when((odd == 1) & (layer < last))
    def _():
        start_outer(0)

    @pl.when(layer == 0)
    def _():
        pl.semaphore_wait(wrap_in, 1)

    @pl.when((odd == 0) & (layer == 0))
    def _():
        start_outer(0)

    mx[...] = stencil(nx, True)
    my[...] = stencil(ny, False)
    plane_sum[...] = jnp.zeros_like(plane_sum)
    zsend[...] = jnp.zeros_like(zsend)
    weights.wait()

    def lateral(n, carry):
        w = occ_ref[n]
        for s in range(depth):
            re = own[n, 0, s]
            im = own[n, 1, s]
            tx = jnp.dot(mx[...], jnp.concatenate([re, im], 1), preferred_element_type=jnp.float32)
            ty = jnp.dot(jnp.concatenate([re, im], 0), my[...], preferred_element_type=jnp.float32)
            wre = re.astype(jnp.float32) * w
            wim = im.astype(jnp.float32) * w
            plane_sum[0, s] += wre * tx[:, ny:] - wim * tx[:, :ny]
            plane_sum[1, s] += wre * ty[nx:] - wim * ty[:nx]
        return carry

    lax.fori_loop(0, bands, lateral, 0)

    def to_peer(k):
        peer = lax.rem(b + k, nb)
        return pltpu.make_async_remote_copy(
            src_ref=plane_sum.at[:, :, pl.ds(pl.multiple_of(peer * rows, rows), rows), :],
            dst_ref=plane_recv.at[k - 1],
            send_sem=sent,
            recv_sem=plane_recv_sem,
            device_id={"band": peer, "grid": g},
        )

    for k in range(1, nb):
        to_peer(k).start()

    for j in range(nb):
        to_mate(j, 0).wait_recv()
        by_wrap(wraps_ahead, j, lambda stop: to_inner(j, stop).start())

    @pl.when(wraps_ahead)
    def _():
        for j in range(nb - HELD, nb):
            by_wrap(wraps, j, lambda start: to_outer(j, start).start())

    mine = pl.ds(pl.multiple_of(b * rows, rows), rows)
    summed = plane_sum[:, :, mine, :]
    bytes_of(plane_recv, plane_recv_sem).wait_recv()
    for k in range(1, nb):
        summed = summed + plane_recv[k - 1]
    out_ref[1:3] = summed * (1.0 / 12.0)

    first = odd
    second = 1 - odd
    sign = turn.astype(jnp.float32)
    zero = jnp.zeros((half, ny), jnp.float32)

    def fields_of(held, n):
        return [tuple(held(n, q, p) for q in (0, 1)) for p in (first, second)]

    def bonds(n, low, high, sums):
        w = occ_ref[n] * sign
        low = [(re * w, im * w) for re, im in low]
        pairs = ((1, 0), (0, 0), (1, 1))
        return tuple(
            total + (low[i][0] * high[k][1] - low[i][1] * high[k][0]) for total, (i, k) in zip(sums, pairs)
        )

    def at_home(j):
        return lambda n, q, p: own[n, q, p, rows_of(j, odd), :].astype(jnp.float32)

    def at_mate(j):
        return lambda n, q, p: mate[j, n, q, p].astype(jnp.float32)

    def core_part(j):
        def step(n, sums):
            low, high = fields_of(at_home(j), n), fields_of(at_mate(j), n)
            w = occ_ref[n] * sign
            inside = tuple(
                total + (slab[0][0] * w * slab[1][1] - slab[0][1] * w * slab[1][0])
                for total, slab in zip(sums[3:], (low, high))
            )
            return bonds(n, low, high, sums[:3]) + inside

        n12, f02, f13, n01, n23 = lax.fori_loop(0, bands, step, (zero,) * 5, unroll=4)
        zsend[j, 0, first] += 8.0 * n01 - f02
        zsend[j, 0, second] += 8.0 * (n01 + n12) - f13
        zsend[j, 2, first] += 8.0 * (n12 + n23) - f02
        zsend[j, 2, second] += 8.0 * n23 - f13

    def straight_part(j):
        def step(n, sums):
            far = fields_of(lambda n, q, p: outer[j, n - split + 1, q, p].astype(jnp.float32), n)
            return bonds(n, fields_of(at_mate(j), n), far, sums)

        sums = lax.fori_loop(split, bands, step, (zero,) * 3, unroll=True)
        if j < max(MIXED):
            sums = lax.fori_loop(split - shifted(wraps_ahead, j), split, step, sums)
        n34, f24, f35 = sums
        zsend[j, 2, first] += -f24
        zsend[j, 2, second] += 8.0 * n34 - f35
        zsend[j, 3, first] = 8.0 * n34 - f24
        zsend[j, 3, second] = -f35

    def passed_part(j):
        def step(n, sums):
            far = fields_of(lambda n, q, p: inner[j, n, q, p].astype(jnp.float32), n)
            return bonds(n, far, fields_of(at_home(j), n), sums)

        always = split - (j < max(MIXED))
        sums = lax.fori_loop(0, always, step, (zero,) * 3, unroll=True)
        if j < max(MIXED):
            sums = lax.fori_loop(always, split - shifted(wraps, j), step, sums)
        n10, f20, f11 = sums
        zsend[j, 0, first] += 8.0 * n10 - f20
        zsend[j, 0, second] += -f11
        zsend[j, 1, first] = -f20
        zsend[j, 1, second] = 8.0 * n10 - f11

    def to_inbox(j, role):
        slot = lax.rem(b - j - 1 + nb, nb)
        return pltpu.make_async_remote_copy(
            src_ref=zsend.at[j, role],
            dst_ref=inbox.at[role, slot],
            send_sem=sent,
            recv_sem=inbox_recv.at[role % 2 + role // 3],
            device_id={"band": j, "grid": g},
        )

    def to_final(j, role):
        return pltpu.make_async_remote_copy(
            src_ref=zsend.at[j, role],
            dst_ref=final.at[role * nb + b],
            send_sem=sent,
            recv_sem=final_recv,
            device_id={"band": j, "grid": (g, side, partner, ahead)[role]},
        )

    def arrive_mate(j):
        to_mate(j, 1).wait_recv()

    def arrive_outer(j):
        by_wrap(wraps_ahead, j, lambda start: to_outer(j, start).wait_recv())

    def arrive_inner(j):
        by_wrap(wraps, j, lambda stop: to_inner(j, stop).wait_recv())

    def finish(j):
        @pl.when(b == j)
        def _():
            for part, roles in ((2, (3,)), (1, (1,)), (0, (0, 2))):
                bytes_of(inbox.at[pl.ds(0, len(roles))], inbox_recv.at[part]).wait_recv()
                for role in roles:
                    zsend[j, role] = zsend[j, role] + sum(inbox[role, slot] for slot in range(nb - 1))
                    if role:
                        to_final(j, role).start()

    for j in range(relayed):
        arrive_mate(j)
        core_part(j)
        arrive_outer(j)
        straight_part(j)

        @pl.when(b != j)
        def _():
            to_inbox(j, 3).start()

        arrive_inner(j)
        passed_part(j)

        @pl.when(b != j)
        def _():
            for role in (1, 2, 0):
                to_inbox(j, role).start()

        if j:
            finish(j - 1)

    def send_own(j):
        @pl.when(b != j)
        def _():
            to_final(j, 0).start()

    for j in range(relayed, nb - 1):
        arrive_mate(j)
        if j > relayed:
            to_final(j - 1, 2).start()
        core_part(j)
        arrive_outer(j)
        straight_part(j)
        to_final(j, 3).start()
        arrive_inner(j)
        passed_part(j)
        to_final(j, 1).start()
        send_own(j)

    end = nb - 1

    @pl.when(wraps)
    def _():
        arrive_inner(end)
        passed_part(end)
        to_final(end, 1).start()

    finish(relayed - 1)
    arrive_mate(end)
    to_final(end - 1, 2).start()

    @pl.when(wraps_ahead)
    def _():
        arrive_outer(end)
        straight_part(end)
        to_final(end, 3).start()

    core_part(end)

    @pl.when(wraps)
    def _():
        send_own(end)

    @pl.when(wraps_ahead)
    def _():
        to_final(end, 2).start()

    @pl.when(jnp.logical_not(wraps))
    def _():
        arrive_inner(end)
        passed_part(end)
        to_final(end, 1).start()
        send_own(end)

    @pl.when(jnp.logical_not(wraps_ahead))
    def _():
        arrive_outer(end)
        straight_part(end)
        to_final(end, 3).start()
        to_final(end, 2).start()

    near = pl.ds(pl.multiple_of(odd * half, half), half)
    away = pl.ds(pl.multiple_of((1 - odd) * half, half), half)

    @pl.when(b >= relayed)
    def _():
        bytes_of(final.at[pl.ds(0, 4 * nb - 1)], final_recv).wait_recv()
        home = zsend[b, 0] + sum(final[lax.rem(b + k, nb)] for k in range(1, nb))
        out_ref[0, :, near, :] = (home + sum(final[3 * nb + k] for k in range(nb))) * (1.0 / 12.0)
        out_ref[0, :, away, :] = sum(final[2 * nb + k] + final[nb + k] for k in range(nb)) * (1.0 / 12.0)

    @pl.when(b < relayed)
    def _():
        bytes_of(final.at[pl.ds(0, 3)], final_recv).wait_recv()
        out_ref[0, :, near, :] = (zsend[b, 0] + final[3 * nb + b]) * (1.0 / 12.0)
        out_ref[0, :, away, :] = (final[2 * nb + b] + final[nb + b]) * (1.0 / 12.0)

    units = 2 * nb * bands + 8 * nb - 5
    for parity in (0, 1):
        for extra, case in (
            (-MIXED[parity], wraps),
            (MIXED[parity], wraps_ahead),
            (0, jnp.logical_not(wraps | wraps_ahead)),
        ):
            @pl.when((odd == parity) & case)
            def _():
                bytes_of(measure.at[pl.ds(0, units + extra)], sent).wait_send()


def solution(mesh):
    nb = mesh.shape["band"]
    ng = mesh.shape["grid"]

    def per_device(orbitals, occupations):
        bands, _, depth, nx, ny = orbitals.shape
        rows = nx // nb
        half = rows // 2
        if depth != 2 or nb % 2 or nb < 4 or ng % 2 or ng < 6 or half % TILE:
            raise ValueError("unsupported sizes")
        f32, bf16 = jnp.float32, jnp.bfloat16
        dma = pltpu.SemaphoreType.DMA
        return pl.pallas_call(
            functools.partial(kernel, nb, ng),
            out_shape=jax.ShapeDtypeStruct((3, depth, rows, ny), f32),
            in_specs=[
                pl.BlockSpec(memory_space=pltpu.HBM),
                pl.BlockSpec(memory_space=pltpu.HBM),
            ],
            out_specs=pl.BlockSpec(memory_space=pltpu.VMEM),
            scratch_shapes=[
                pltpu.SMEM((bands,), f32),
                pltpu.VMEM((bands, 2, depth, nx, ny), bf16),
                pltpu.VMEM((nb, bands, 2, depth, half, ny), bf16),
                pltpu.VMEM((nb, bands - bands // 2 + 1, 2, depth, half, ny), bf16),
                pltpu.VMEM((nb, bands // 2, 2, depth, half, ny), bf16),
                pltpu.VMEM((nx, nx), bf16),
                pltpu.VMEM((ny, ny), bf16),
                pltpu.VMEM((2, depth, nx, ny), f32),
                pltpu.VMEM((nb - 1, 2, depth, rows, ny), f32),
                pltpu.VMEM((nb, 4, depth, half, ny), f32),
                pltpu.VMEM((4, nb - 1, depth, half, ny), f32),
                pltpu.VMEM((4 * nb, depth, half, ny), f32),
                pltpu.VMEM((2 * nb * bands + 8 * nb - 5 + max(MIXED), depth, half, ny), f32),
                dma,
                dma,
                dma,
                dma((2, nb)),
                dma((nb,)),
                dma((nb,)),
                dma,
                dma((3,)),
                dma,
                pltpu.SemaphoreType.REGULAR,
                pltpu.SemaphoreType.REGULAR,
            ],
            compiler_params=pltpu.CompilerParams(collective_id=0, has_side_effects=True, vmem_limit_bytes=55000 * 1024),
            name="current",
        )(pltpu.with_memory_space_constraint(occupations, pltpu.HBM), orbitals)

    return jax.shard_map(
        per_device,
        mesh=mesh,
        in_specs=(P("band", None, "grid", None, None), P("band")),
        out_specs=P(None, "grid", "band", None),
        check_vma=False,
    )
```

```python
import functools

import jax
import jax.numpy as jnp
from jax import lax
from jax.experimental import pallas as pl
from jax.experimental.pallas import tpu as pltpu
from jax.sharding import PartitionSpec as P

TILE = 16
MIXED = (3, 1)
HELD = 1


def stencil(n, flipped):
    row = lax.broadcasted_iota(jnp.int32, (n, n), 0)
    col = lax.broadcasted_iota(jnp.int32, (n, n), 1)
    d = col - row if flipped else row - col
    value = jnp.zeros((n, n), jnp.float32)
    for step, weight in ((1, 8.0), (-1, -8.0), (2, -1.0), (-2, 1.0)):
        hit = (d == step) | (d == step - n) | (d == step + n)
        value = jnp.where(hit, weight, value)
    return value.astype(jnp.bfloat16)


def kernel(
    nb, ng, occ_hbm, orb_ref, out_ref,
    occ_ref, own, mate, outer, inner, mx, my, plane_sum, plane_recv, zsend, inbox, final, measure,
    own_sem, sent, mate_recv, outer_recv, inner_recv, plane_recv_sem, inbox_recv, final_recv, answers, wrap_in,
):
    bands, _, depth, nx, ny = orb_ref.shape
    b = lax.axis_index("band")
    g = lax.axis_index("grid")
    odd = lax.rem(g, 2)
    turn = 1 - 2 * odd
    partner = g + turn
    ahead = lax.rem(g + 2 * turn + ng, ng)
    behind = lax.rem(g - 2 * turn + ng, ng)
    side = lax.rem(g - turn + ng, ng)
    layers = ng // 2
    layer = g // 2
    rows = nx // nb
    half = rows // 2
    split = bands // 2
    relayed = nb // 2

    load = pltpu.make_async_copy(orb_ref, own, own_sem)
    load.start()
    weights = pltpu.make_async_copy(occ_hbm, occ_ref, own_sem)

    barrier = pltpu.get_barrier_semaphore()
    last = layers - 1

    def tell(semaphore, band, grid):
        pl.semaphore_signal(semaphore, inc=1, device_id={"band": band, "grid": grid})

    @pl.when(odd == 0)
    def _():
        tell(barrier, b, partner)

    @pl.when(layer < last)
    def _():
        tell(barrier, b, g + 2)

    @pl.when(layer == 0)
    def _():
        tell(barrier, b, g + 2 * last)

    chip = b // 2
    tell(barrier, b + 1 - 2 * lax.rem(b, 2), g)
    for k in range(2, nb):
        @pl.when(2 * chip + k < nb)
        def _():
            tell(barrier, 2 * chip + k, g)

    earlier = odd + (layer > 0).astype(jnp.int32) + (layer == last).astype(jnp.int32) + 2 * chip + 1
    pl.semaphore_wait(barrier, earlier)

    @pl.when(odd == 1)
    def _():
        tell(answers, b, partner)

    @pl.when(layer > 0)
    def _():
        tell(answers, b, g - 2)

    @pl.when(layer == last)
    def _():
        tell(wrap_in, b, g - 2 * last)

    for k in range(1, nb - 1):
        @pl.when(2 * chip - k >= 0)
        def _():
            tell(answers, 2 * chip - k, g)

    def bytes_of(ref, semaphore):
        return pltpu.make_async_remote_copy(
            src_ref=ref, dst_ref=ref, send_sem=semaphore, recv_sem=semaphore, device_id={"band": b, "grid": partner}
        )

    def rows_of(j, parity):
        return pl.ds(pl.multiple_of(j * rows + parity * half, half), half)

    passed, straight = pl.ds(0, split), pl.ds(split, bands - split)

    def to_mate(j, kind, source=None):
        source = own if source is None else source
        part = (passed, straight)[kind]
        return pltpu.make_async_remote_copy(
            src_ref=source.at[part, :, :, rows_of(j, 1 - odd), :],
            dst_ref=mate.at[j, part],
            send_sem=sent,
            recv_sem=mate_recv.at[kind, j],
            device_id={"band": b, "grid": partner},
        )

    def to_outer(j, start, source=None):
        source = own if source is None else source
        part = pl.ds(start, bands - start)
        return pltpu.make_async_remote_copy(
            src_ref=source.at[part, :, :, rows_of(j, odd), :],
            dst_ref=outer.at[j, pl.ds(start - split + 1, bands - start)],
            send_sem=sent,
            recv_sem=outer_recv.at[j],
            device_id={"band": b, "grid": behind},
        )

    def to_inner(j, stop):
        return pltpu.make_async_remote_copy(
            src_ref=mate.at[j, pl.ds(0, stop)],
            dst_ref=inner.at[j, pl.ds(0, stop)],
            send_sem=sent,
            recv_sem=inner_recv.at[j],
            device_id={"band": b, "grid": ahead},
        )

    def by_wrap(wrapping, j, act):
        if j >= max(MIXED):
            act(split)
            return
        plain = wrapping
        for parity in (0, 1):
            if j >= MIXED[parity]:
                plain = plain | (odd == parity)

        @pl.when(plain)
        def _():
            act(split)

        @pl.when(jnp.logical_not(plain))
        def _():
            act(split - 1)

    def shifted(wrapping, j):
        by_parity = jnp.where(odd == 1, int(j < MIXED[1]), int(j < MIXED[0]))
        return jnp.where(wrapping, 0, by_parity)

    wraps = ((odd == 0) & (layer == 0)) | ((odd == 1) & (layer == layers - 1))
    wraps_ahead = ((odd == 0) & (layer == layers - 1)) | ((odd == 1) & (layer == 0))
    def start_mate(skip):
        for kind in (0, 1):
            for j in range(nb):
                if kind or j >= skip:
                    to_mate(j, kind).start()

    def start_outer(skip):
        for j in range(skip, nb - HELD):
            by_wrap(wraps, j, lambda start: to_outer(j, start).start())

        @pl.when(jnp.logical_not(wraps_ahead))
        def _():
            for j in range(nb - HELD, nb):
                by_wrap(wraps, j, lambda start: to_outer(j, start).start())

    known = ((odd == 0) & (layer > 0)) | ((odd == 1) & (layer == last))

    @pl.when(odd == 1)
    def _():
        to_mate(0, 0, orb_ref).start()

    @pl.when(known)
    def _():
        by_wrap(wraps, 0, lambda start: to_outer(0, start, orb_ref).start())

    load.wait()
    weights.start()

    @pl.when(known)
    def _():
        start_outer(1)

    later = nb - 2 * chip - 2 + (1 - odd) + (layer < last).astype(jnp.int32)

    @pl.when(later > 0)
    def _():
        pl.semaphore_wait(answers, later)

    @pl.when(odd == 1)
    def _():
        start_mate(1)

    @pl.when(odd == 0)
    def _():
        start_mate(0)

    @pl.when((odd == 1) & (layer < last))
    def _():
        start_outer(0)

    @pl.when(layer == 0)
    def _():
        pl.semaphore_wait(wrap_in, 1)

    @pl.when((odd == 0) & (layer == 0))
    def _():
        start_outer(0)

    mx[...] = stencil(nx, True)
    my[...] = stencil(ny, False)
    plane_sum[...] = jnp.zeros_like(plane_sum)
    zsend[...] = jnp.zeros_like(zsend)
    weights.wait()

    def lateral(n, carry):
        w = occ_ref[n]
        for s in range(depth):
            re = own[n, 0, s]
            im = own[n, 1, s]
            tx = jnp.dot(mx[...], jnp.concatenate([re, im], 1), preferred_element_type=jnp.float32)
            ty = jnp.dot(jnp.concatenate([re, im], 0), my[...], preferred_element_type=jnp.float32)
            wre = re.astype(jnp.float32) * w
            wim = im.astype(jnp.float32) * w
            plane_sum[0, s] += wre * tx[:, ny:] - wim * tx[:, :ny]
            plane_sum[1, s] += wre * ty[nx:] - wim * ty[:nx]
        return carry

    lax.fori_loop(0, bands, lateral, 0)

    def to_peer(k):
        peer = lax.rem(b + k, nb)
        return pltpu.make_async_remote_copy(
            src_ref=plane_sum.at[:, :, pl.ds(pl.multiple_of(peer * rows, rows), rows), :],
            dst_ref=plane_recv.at[k - 1],
            send_sem=sent,
            recv_sem=plane_recv_sem,
            device_id={"band": peer, "grid": g},
        )

    for k in range(1, nb):
        to_peer(k).start()

    for j in range(nb):
        to_mate(j, 0).wait_recv()
        by_wrap(wraps_ahead, j, lambda stop: to_inner(j, stop).start())

    def start_held(now):
        @pl.when(wraps_ahead & now)
        def _():
            for j in range(nb - HELD, nb):
                by_wrap(wraps, j, lambda start: to_outer(j, start).start())

    start_held(b > 0)

    mine = pl.ds(pl.multiple_of(b * rows, rows), rows)
    summed = plane_sum[:, :, mine, :]
    bytes_of(plane_recv, plane_recv_sem).wait_recv()
    for k in range(1, nb):
        summed = summed + plane_recv[k - 1]
    out_ref[1:3] = summed * (1.0 / 12.0)

    first = odd
    second = 1 - odd
    sign = turn.astype(jnp.float32)
    zero = jnp.zeros((half, ny), jnp.float32)

    def fields_of(held, n):
        return [tuple(held(n, q, p) for q in (0, 1)) for p in (first, second)]

    def bonds(n, low, high, sums):
        w = occ_ref[n] * sign
        low = [(re * w, im * w) for re, im in low]
        pairs = ((1, 0), (0, 0), (1, 1))
        return tuple(
            total + (low[i][0] * high[k][1] - low[i][1] * high[k][0]) for total, (i, k) in zip(sums, pairs)
        )

    def at_home(j):
        return lambda n, q, p: own[n, q, p, rows_of(j, odd), :].astype(jnp.float32)

    def at_mate(j):
        return lambda n, q, p: mate[j, n, q, p].astype(jnp.float32)

    def core_part(j):
        def step(n, sums):
            low, high = fields_of(at_home(j), n), fields_of(at_mate(j), n)
            w = occ_ref[n] * sign
            inside = tuple(
                total + (slab[0][0] * w * slab[1][1] - slab[0][1] * w * slab[1][0])
                for total, slab in zip(sums[3:], (low, high))
            )
            return bonds(n, low, high, sums[:3]) + inside

        n12, f02, f13, n01, n23 = lax.fori_loop(0, bands, step, (zero,) * 5, unroll=4)
        zsend[j, 0, first] += 8.0 * n01 - f02
        zsend[j, 0, second] += 8.0 * (n01 + n12) - f13
        zsend[j, 2, first] += 8.0 * (n12 + n23) - f02
        zsend[j, 2, second] += 8.0 * n23 - f13

    def straight_part(j):
        def step(n, sums):
            far = fields_of(lambda n, q, p: outer[j, n - split + 1, q, p].astype(jnp.float32), n)
            return bonds(n, fields_of(at_mate(j), n), far, sums)

        sums = lax.fori_loop(split, bands, step, (zero,) * 3, unroll=True)
        if j < max(MIXED):
            sums = lax.fori_loop(split - shifted(wraps_ahead, j), split, step, sums)
        n34, f24, f35 = sums
        zsend[j, 2, first] += -f24
        zsend[j, 2, second] += 8.0 * n34 - f35
        zsend[j, 3, first] = 8.0 * n34 - f24
        zsend[j, 3, second] = -f35

    def passed_part(j):
        def step(n, sums):
            far = fields_of(lambda n, q, p: inner[j, n, q, p].astype(jnp.float32), n)
            return bonds(n, far, fields_of(at_home(j), n), sums)

        always = split - (j < max(MIXED))
        sums = lax.fori_loop(0, always, step, (zero,) * 3, unroll=True)
        if j < max(MIXED):
            sums = lax.fori_loop(always, split - shifted(wraps, j), step, sums)
        n10, f20, f11 = sums
        zsend[j, 0, first] += 8.0 * n10 - f20
        zsend[j, 0, second] += -f11
        zsend[j, 1, first] = -f20
        zsend[j, 1, second] = 8.0 * n10 - f11

    def to_inbox(j, role):
        slot = lax.rem(b - j - 1 + nb, nb)
        return pltpu.make_async_remote_copy(
            src_ref=zsend.at[j, role],
            dst_ref=inbox.at[role, slot],
            send_sem=sent,
            recv_sem=inbox_recv.at[role % 2 + role // 3],
            device_id={"band": j, "grid": g},
        )

    def to_final(j, role):
        return pltpu.make_async_remote_copy(
            src_ref=zsend.at[j, role],
            dst_ref=final.at[role * nb + b],
            send_sem=sent,
            recv_sem=final_recv,
            device_id={"band": j, "grid": (g, side, partner, ahead)[role]},
        )

    def arrive_mate(j):
        to_mate(j, 1).wait_recv()

    def arrive_outer(j):
        by_wrap(wraps_ahead, j, lambda start: to_outer(j, start).wait_recv())

    def arrive_inner(j):
        by_wrap(wraps, j, lambda stop: to_inner(j, stop).wait_recv())

    def finish(j):
        @pl.when(b == j)
        def _():
            for part, roles in ((2, (3,)), (1, (1,)), (0, (0, 2))):
                bytes_of(inbox.at[pl.ds(0, len(roles))], inbox_recv.at[part]).wait_recv()
                for role in roles:
                    zsend[j, role] = zsend[j, role] + sum(inbox[role, slot] for slot in range(nb - 1))
                    if role:
                        to_final(j, role).start()

    for j in range(relayed):
        arrive_mate(j)
        core_part(j)
        arrive_outer(j)
        straight_part(j)

        @pl.when(b != j)
        def _():
            to_inbox(j, 3).start()

        arrive_inner(j)
        passed_part(j)

        @pl.when(b != j)
        def _():
            for role in (1, 2, 0):
                to_inbox(j, role).start()

        if j:
            finish(j - 1)
            if j == 1:
                start_held(b == 0)

    def send_own(j):
        @pl.when(b != j)
        def _():
            to_final(j, 0).start()

    for j in range(relayed, nb - 1):
        arrive_mate(j)
        if j > relayed:
            to_final(j - 1, 2).start()
        core_part(j)
        arrive_outer(j)
        straight_part(j)
        to_final(j, 3).start()
        arrive_inner(j)
        passed_part(j)
        to_final(j, 1).start()
        send_own(j)

    end = nb - 1

    @pl.when(wraps)
    def _():
        arrive_inner(end)
        passed_part(end)
        to_final(end, 1).start()

    finish(relayed - 1)
    arrive_mate(end)
    to_final(end - 1, 2).start()

    @pl.when(wraps_ahead)
    def _():
        arrive_outer(end)
        straight_part(end)
        to_final(end, 3).start()

    core_part(end)

    @pl.when(wraps)
    def _():
        send_own(end)

    @pl.when(wraps_ahead)
    def _():
        to_final(end, 2).start()

    @pl.when(jnp.logical_not(wraps))
    def _():
        arrive_inner(end)
        passed_part(end)
        to_final(end, 1).start()
        send_own(end)

    @pl.when(jnp.logical_not(wraps_ahead))
    def _():
        arrive_outer(end)
        straight_part(end)
        to_final(end, 3).start()
        to_final(end, 2).start()

    near = pl.ds(pl.multiple_of(odd * half, half), half)
    away = pl.ds(pl.multiple_of((1 - odd) * half, half), half)

    @pl.when(b >= relayed)
    def _():
        bytes_of(final.at[pl.ds(0, 4 * nb - 1)], final_recv).wait_recv()
        home = zsend[b, 0] + sum(final[lax.rem(b + k, nb)] for k in range(1, nb))
        out_ref[0, :, near, :] = (home + sum(final[3 * nb + k] for k in range(nb))) * (1.0 / 12.0)
        out_ref[0, :, away, :] = sum(final[2 * nb + k] + final[nb + k] for k in range(nb)) * (1.0 / 12.0)

    @pl.when(b < relayed)
    def _():
        bytes_of(final.at[pl.ds(0, 3)], final_recv).wait_recv()
        out_ref[0, :, near, :] = (zsend[b, 0] + final[3 * nb + b]) * (1.0 / 12.0)
        out_ref[0, :, away, :] = (final[2 * nb + b] + final[nb + b]) * (1.0 / 12.0)

    units = 2 * nb * bands + 8 * nb - 5
    for parity in (0, 1):
        for extra, case in (
            (-MIXED[parity], wraps),
            (MIXED[parity], wraps_ahead),
            (0, jnp.logical_not(wraps | wraps_ahead)),
        ):
            @pl.when((odd == parity) & case)
            def _():
                bytes_of(measure.at[pl.ds(0, units + extra)], sent).wait_send()


def solution(mesh):
    nb = mesh.shape["band"]
    ng = mesh.shape["grid"]

    def per_device(orbitals, occupations):
        bands, _, depth, nx, ny = orbitals.shape
        rows = nx // nb
        half = rows // 2
        if depth != 2 or nb % 2 or nb < 4 or ng % 2 or ng < 6 or half % TILE:
            raise ValueError("unsupported sizes")
        f32, bf16 = jnp.float32, jnp.bfloat16
        dma = pltpu.SemaphoreType.DMA
        return pl.pallas_call(
            functools.partial(kernel, nb, ng),
            out_shape=jax.ShapeDtypeStruct((3, depth, rows, ny), f32),
            in_specs=[
                pl.BlockSpec(memory_space=pltpu.HBM),
                pl.BlockSpec(memory_space=pltpu.HBM),
            ],
            out_specs=pl.BlockSpec(memory_space=pltpu.VMEM),
            scratch_shapes=[
                pltpu.SMEM((bands,), f32),
                pltpu.VMEM((bands, 2, depth, nx, ny), bf16),
                pltpu.VMEM((nb, bands, 2, depth, half, ny), bf16),
                pltpu.VMEM((nb, bands - bands // 2 + 1, 2, depth, half, ny), bf16),
                pltpu.VMEM((nb, bands // 2, 2, depth, half, ny), bf16),
                pltpu.VMEM((nx, nx), bf16),
                pltpu.VMEM((ny, ny), bf16),
                pltpu.VMEM((2, depth, nx, ny), f32),
                pltpu.VMEM((nb - 1, 2, depth, rows, ny), f32),
                pltpu.VMEM((nb, 4, depth, half, ny), f32),
                pltpu.VMEM((4, nb - 1, depth, half, ny), f32),
                pltpu.VMEM((4 * nb, depth, half, ny), f32),
                pltpu.VMEM((2 * nb * bands + 8 * nb - 5 + max(MIXED), depth, half, ny), f32),
                dma,
                dma,
                dma((2, nb)),
                dma((nb,)),
                dma((nb,)),
                dma,
                dma((3,)),
                dma,
                pltpu.SemaphoreType.REGULAR,
                pltpu.SemaphoreType.REGULAR,
            ],
            compiler_params=pltpu.CompilerParams(collective_id=0, has_side_effects=True, vmem_limit_bytes=55000 * 1024),
            name="current",
        )(pltpu.with_memory_space_constraint(occupations, pltpu.HBM), orbitals)

    return jax.shard_map(
        per_device,
        mesh=mesh,
        in_specs=(P("band", None, "grid", None, None), P("band")),
        out_specs=P(None, "grid", "band", None),
        check_vma=False,
    )
```

```python
import functools

import jax
import jax.numpy as jnp
from jax import lax
from jax.experimental import pallas as pl
from jax.experimental.pallas import tpu as pltpu
from jax.sharding import PartitionSpec as P

TILE = 16
MIXED = (3, 1)
HELD = 1


def stencil(n, flipped):
    row = lax.broadcasted_iota(jnp.int32, (n, n), 0)
    col = lax.broadcasted_iota(jnp.int32, (n, n), 1)
    d = col - row if flipped else row - col
    value = jnp.zeros((n, n), jnp.float32)
    for step, weight in ((1, 8.0), (-1, -8.0), (2, -1.0), (-2, 1.0)):
        hit = (d == step) | (d == step - n) | (d == step + n)
        value = jnp.where(hit, weight, value)
    return value.astype(jnp.bfloat16)


def kernel(
    nb, ng, occ_hbm, orb_ref, out_ref,
    occ_ref, own, mate, outer, inner, mx, my, plane_sum, plane_recv, zsend, inbox, final, measure,
    own_sem, sent, mate_recv, outer_recv, inner_recv, plane_recv_sem, inbox_recv, final_recv, answers, wrap_in,
):
    bands, _, depth, nx, ny = orb_ref.shape
    b = lax.axis_index("band")
    g = lax.axis_index("grid")
    odd = lax.rem(g, 2)
    turn = 1 - 2 * odd
    partner = g + turn
    ahead = lax.rem(g + 2 * turn + ng, ng)
    behind = lax.rem(g - 2 * turn + ng, ng)
    side = lax.rem(g - turn + ng, ng)
    layers = ng // 2
    layer = g // 2
    rows = nx // nb
    half = rows // 2
    split = bands // 2
    relayed = nb // 2

    load = pltpu.make_async_copy(orb_ref, own, own_sem)
    load.start()
    weights = pltpu.make_async_copy(occ_hbm, occ_ref, own_sem)

    barrier = pltpu.get_barrier_semaphore()
    last = layers - 1

    def tell(semaphore, band, grid):
        pl.semaphore_signal(semaphore, inc=1, device_id={"band": band, "grid": grid})

    @pl.when(odd == 0)
    def _():
        tell(barrier, b, partner)

    @pl.when(layer < last)
    def _():
        tell(barrier, b, g + 2)

    @pl.when(layer == 0)
    def _():
        tell(barrier, b, g + 2 * last)

    chip = b // 2
    tell(barrier, b + 1 - 2 * lax.rem(b, 2), g)
    for k in range(2, nb):
        @pl.when(2 * chip + k < nb)
        def _():
            tell(barrier, 2 * chip + k, g)

    earlier = odd + (layer > 0).astype(jnp.int32) + (layer == last).astype(jnp.int32) + 2 * chip + 1
    pl.semaphore_wait(barrier, earlier)

    @pl.when(odd == 1)
    def _():
        tell(answers, b, partner)

    @pl.when(layer > 0)
    def _():
        tell(answers, b, g - 2)

    @pl.when(layer == last)
    def _():
        tell(wrap_in, b, g - 2 * last)

    for k in range(1, nb - 1):
        @pl.when(2 * chip - k >= 0)
        def _():
            tell(answers, 2 * chip - k, g)

    def bytes_of(ref, semaphore):
        return pltpu.make_async_remote_copy(
            src_ref=ref, dst_ref=ref, send_sem=semaphore, recv_sem=semaphore, device_id={"band": b, "grid": partner}
        )

    def rows_of(j, parity):
        return pl.ds(pl.multiple_of(j * rows + parity * half, half), half)

    passed, straight = pl.ds(0, split), pl.ds(split, bands - split)

    def to_mate(j, kind, source=None):
        source = own if source is None else source
        part = (passed, straight)[kind]
        return pltpu.make_async_remote_copy(
            src_ref=source.at[part, :, :, rows_of(j, 1 - odd), :],
            dst_ref=mate.at[j, part],
            send_sem=sent,
            recv_sem=mate_recv.at[kind, j],
            device_id={"band": b, "grid": partner},
        )

    def to_outer(j, start, source=None):
        source = own if source is None else source
        part = pl.ds(start, bands - start)
        return pltpu.make_async_remote_copy(
            src_ref=source.at[part, :, :, rows_of(j, odd), :],
            dst_ref=outer.at[j, pl.ds(start - split + 1, bands - start)],
            send_sem=sent,
            recv_sem=outer_recv.at[j],
            device_id={"band": b, "grid": behind},
        )

    def to_inner(j, stop):
        return pltpu.make_async_remote_copy(
            src_ref=mate.at[j, pl.ds(0, stop)],
            dst_ref=inner.at[j, pl.ds(0, stop)],
            send_sem=sent,
            recv_sem=inner_recv.at[j],
            device_id={"band": b, "grid": ahead},
        )

    def by_wrap(wrapping, j, act):
        if j >= max(MIXED):
            act(split)
            return
        plain = wrapping
        for parity in (0, 1):
            if j >= MIXED[parity]:
                plain = plain | (odd == parity)

        @pl.when(plain)
        def _():
            act(split)

        @pl.when(jnp.logical_not(plain))
        def _():
            act(split - 1)

    def shifted(wrapping, j):
        by_parity = jnp.where(odd == 1, int(j < MIXED[1]), int(j < MIXED[0]))
        return jnp.where(wrapping, 0, by_parity)

    wraps = ((odd == 0) & (layer == 0)) | ((odd == 1) & (layer == layers - 1))
    wraps_ahead = ((odd == 0) & (layer == layers - 1)) | ((odd == 1) & (layer == 0))
    def start_mate(skip):
        for kind in (0, 1):
            for j in range(nb):
                if kind or j >= skip:
                    to_mate(j, kind).start()

    def start_outer(skip):
        for j in range(skip, nb - HELD):
            by_wrap(wraps, j, lambda start: to_outer(j, start).start())

        @pl.when(jnp.logical_not(wraps_ahead))
        def _():
            for j in range(nb - HELD, nb):
                by_wrap(wraps, j, lambda start: to_outer(j, start).start())

    known = ((odd == 0) & (layer > 0)) | ((odd == 1) & (layer == last))

    @pl.when(odd == 1)
    def _():
        to_mate(0, 0, orb_ref).start()

    @pl.when(known)
    def _():
        by_wrap(wraps, 0, lambda start: to_outer(0, start, orb_ref).start())

    load.wait()
    weights.start()

    @pl.when(known)
    def _():
        start_outer(1)

    later = nb - 2 * chip - 2 + (1 - odd) + (layer < last).astype(jnp.int32)

    @pl.when(later > 0)
    def _():
        pl.semaphore_wait(answers, later)

    @pl.when(odd == 1)
    def _():
        start_mate(1)

    @pl.when(odd == 0)
    def _():
        start_mate(0)

    @pl.when((odd == 1) & (layer < last))
    def _():
        start_outer(0)

    @pl.when(layer == 0)
    def _():
        pl.semaphore_wait(wrap_in, 1)

    @pl.when((odd == 0) & (layer == 0))
    def _():
        start_outer(0)

    mx[...] = stencil(nx, True)
    my[...] = stencil(ny, False)
    plane_sum[...] = jnp.zeros_like(plane_sum)
    zsend[...] = jnp.zeros_like(zsend)
    weights.wait()

    def lateral(n, carry):
        w = occ_ref[n]
        for s in range(depth):
            re = own[n, 0, s]
            im = own[n, 1, s]
            tx = jnp.dot(mx[...], jnp.concatenate([re, im], 1), preferred_element_type=jnp.float32)
            ty = jnp.dot(jnp.concatenate([re, im], 0), my[...], preferred_element_type=jnp.float32)
            wre = re.astype(jnp.float32) * w
            wim = im.astype(jnp.float32) * w
            plane_sum[0, s] += wre * tx[:, ny:] - wim * tx[:, :ny]
            plane_sum[1, s] += wre * ty[nx:] - wim * ty[:nx]
        return carry

    lax.fori_loop(0, bands, lateral, 0)

    def to_peer(k):
        peer = lax.rem(b + k, nb)
        return pltpu.make_async_remote_copy(
            src_ref=plane_sum.at[:, :, pl.ds(pl.multiple_of(peer * rows, rows), rows), :],
            dst_ref=plane_recv.at[k - 1],
            send_sem=sent,
            recv_sem=plane_recv_sem,
            device_id={"band": peer, "grid": g},
        )

    for k in range(1, nb):
        to_peer(k).start()

    for j in range(nb):
        to_mate(j, 0).wait_recv()
        by_wrap(wraps_ahead, j, lambda stop: to_inner(j, stop).start())

    def start_held(now):
        @pl.when(wraps_ahead & now)
        def _():
            for j in range(nb - HELD, nb):
                by_wrap(wraps, j, lambda start: to_outer(j, start).start())

    start_held((b > 0) | (odd == 1))

    mine = pl.ds(pl.multiple_of(b * rows, rows), rows)
    summed = plane_sum[:, :, mine, :]
    bytes_of(plane_recv, plane_recv_sem).wait_recv()
    for k in range(1, nb):
        summed = summed + plane_recv[k - 1]
    out_ref[1:3] = summed * (1.0 / 12.0)

    first = odd
    second = 1 - odd
    sign = turn.astype(jnp.float32)
    zero = jnp.zeros((half, ny), jnp.float32)

    def fields_of(held, n):
        return [tuple(held(n, q, p) for q in (0, 1)) for p in (first, second)]

    def bonds(n, low, high, sums):
        w = occ_ref[n] * sign
        low = [(re * w, im * w) for re, im in low]
        pairs = ((1, 0), (0, 0), (1, 1))
        return tuple(
            total + (low[i][0] * high[k][1] - low[i][1] * high[k][0]) for total, (i, k) in zip(sums, pairs)
        )

    def at_home(j):
        return lambda n, q, p: own[n, q, p, rows_of(j, odd), :].astype(jnp.float32)

    def at_mate(j):
        return lambda n, q, p: mate[j, n, q, p].astype(jnp.float32)

    def core_part(j):
        def step(n, sums):
            low, high = fields_of(at_home(j), n), fields_of(at_mate(j), n)
            w = occ_ref[n] * sign
            inside = tuple(
                total + (slab[0][0] * w * slab[1][1] - slab[0][1] * w * slab[1][0])
                for total, slab in zip(sums[3:], (low, high))
            )
            return bonds(n, low, high, sums[:3]) + inside

        n12, f02, f13, n01, n23 = lax.fori_loop(0, bands, step, (zero,) * 5, unroll=4)
        zsend[j, 0, first] += 8.0 * n01 - f02
        zsend[j, 0, second] += 8.0 * (n01 + n12) - f13
        zsend[j, 2, first] += 8.0 * (n12 + n23) - f02
        zsend[j, 2, second] += 8.0 * n23 - f13

    def straight_part(j):
        def step(n, sums):
            far = fields_of(lambda n, q, p: outer[j, n - split + 1, q, p].astype(jnp.float32), n)
            return bonds(n, fields_of(at_mate(j), n), far, sums)

        sums = lax.fori_loop(split, bands, step, (zero,) * 3, unroll=True)
        if j < max(MIXED):
            sums = lax.fori_loop(split - shifted(wraps_ahead, j), split, step, sums)
        n34, f24, f35 = sums
        zsend[j, 2, first] += -f24
        zsend[j, 2, second] += 8.0 * n34 - f35
        zsend[j, 3, first] = 8.0 * n34 - f24
        zsend[j, 3, second] = -f35

    def passed_part(j):
        def step(n, sums):
            far = fields_of(lambda n, q, p: inner[j, n, q, p].astype(jnp.float32), n)
            return bonds(n, far, fields_of(at_home(j), n), sums)

        always = split - (j < max(MIXED))
        sums = lax.fori_loop(0, always, step, (zero,) * 3, unroll=True)
        if j < max(MIXED):
            sums = lax.fori_loop(always, split - shifted(wraps, j), step, sums)
        n10, f20, f11 = sums
        zsend[j, 0, first] += 8.0 * n10 - f20
        zsend[j, 0, second] += -f11
        zsend[j, 1, first] = -f20
        zsend[j, 1, second] = 8.0 * n10 - f11

    def to_inbox(j, role):
        slot = lax.rem(b - j - 1 + nb, nb)
        return pltpu.make_async_remote_copy(
            src_ref=zsend.at[j, role],
            dst_ref=inbox.at[role, slot],
            send_sem=sent,
            recv_sem=inbox_recv.at[role % 2 + role // 3],
            device_id={"band": j, "grid": g},
        )

    def to_final(j, role):
        return pltpu.make_async_remote_copy(
            src_ref=zsend.at[j, role],
            dst_ref=final.at[role * nb + b],
            send_sem=sent,
            recv_sem=final_recv,
            device_id={"band": j, "grid": (g, side, partner, ahead)[role]},
        )

    def arrive_mate(j):
        to_mate(j, 1).wait_recv()

    def arrive_outer(j):
        by_wrap(wraps_ahead, j, lambda start: to_outer(j, start).wait_recv())

    def arrive_inner(j):
        by_wrap(wraps, j, lambda stop: to_inner(j, stop).wait_recv())

    def finish(j):
        @pl.when(b == j)
        def _():
            for part, roles in ((2, (3,)), (1, (1,)), (0, (0, 2))):
                bytes_of(inbox.at[pl.ds(0, len(roles))], inbox_recv.at[part]).wait_recv()
                for role in roles:
                    zsend[j, role] = zsend[j, role] + sum(inbox[role, slot] for slot in range(nb - 1))
                    if role:
                        to_final(j, role).start()

    for j in range(relayed):
        arrive_mate(j)
        core_part(j)
        arrive_outer(j)
        straight_part(j)

        @pl.when(b != j)
        def _():
            to_inbox(j, 3).start()

        arrive_inner(j)
        passed_part(j)

        @pl.when(b != j)
        def _():
            for role in (1, 2, 0):
                to_inbox(j, role).start()

        if j:
            finish(j - 1)
            if j == 1:
                start_held((b == 0) & (odd == 0))

    def send_own(j):
        @pl.when(b != j)
        def _():
            to_final(j, 0).start()

    for j in range(relayed, nb - 1):
        arrive_mate(j)
        if j > relayed:
            to_final(j - 1, 2).start()
        core_part(j)
        arrive_outer(j)
        straight_part(j)
        to_final(j, 3).start()
        arrive_inner(j)
        passed_part(j)
        to_final(j, 1).start()
        send_own(j)

    end = nb - 1

    @pl.when(wraps)
    def _():
        arrive_inner(end)
        passed_part(end)
        to_final(end, 1).start()

    finish(relayed - 1)
    arrive_mate(end)
    to_final(end - 1, 2).start()

    @pl.when(wraps_ahead)
    def _():
        arrive_outer(end)
        straight_part(end)
        to_final(end, 3).start()

    core_part(end)

    @pl.when(wraps)
    def _():
        send_own(end)

    @pl.when(wraps_ahead)
    def _():
        to_final(end, 2).start()

    @pl.when(jnp.logical_not(wraps))
    def _():
        arrive_inner(end)
        passed_part(end)
        to_final(end, 1).start()
        send_own(end)

    @pl.when(jnp.logical_not(wraps_ahead))
    def _():
        arrive_outer(end)
        straight_part(end)
        to_final(end, 3).start()
        to_final(end, 2).start()

    near = pl.ds(pl.multiple_of(odd * half, half), half)
    away = pl.ds(pl.multiple_of((1 - odd) * half, half), half)

    @pl.when(b >= relayed)
    def _():
        bytes_of(final.at[pl.ds(0, 4 * nb - 1)], final_recv).wait_recv()
        home = zsend[b, 0] + sum(final[lax.rem(b + k, nb)] for k in range(1, nb))
        out_ref[0, :, near, :] = (home + sum(final[3 * nb + k] for k in range(nb))) * (1.0 / 12.0)
        out_ref[0, :, away, :] = sum(final[2 * nb + k] + final[nb + k] for k in range(nb)) * (1.0 / 12.0)

    @pl.when(b < relayed)
    def _():
        bytes_of(final.at[pl.ds(0, 3)], final_recv).wait_recv()
        out_ref[0, :, near, :] = (zsend[b, 0] + final[3 * nb + b]) * (1.0 / 12.0)
        out_ref[0, :, away, :] = (final[2 * nb + b] + final[nb + b]) * (1.0 / 12.0)

    units = 2 * nb * bands + 8 * nb - 5
    for parity in (0, 1):
        for extra, case in (
            (-MIXED[parity], wraps),
            (MIXED[parity], wraps_ahead),
            (0, jnp.logical_not(wraps | wraps_ahead)),
        ):
            @pl.when((odd == parity) & case)
            def _():
                bytes_of(measure.at[pl.ds(0, units + extra)], sent).wait_send()


def solution(mesh):
    nb = mesh.shape["band"]
    ng = mesh.shape["grid"]

    def per_device(orbitals, occupations):
        bands, _, depth, nx, ny = orbitals.shape
        rows = nx // nb
        half = rows // 2
        if depth != 2 or nb % 2 or nb < 4 or ng % 2 or ng < 6 or half % TILE:
            raise ValueError("unsupported sizes")
        f32, bf16 = jnp.float32, jnp.bfloat16
        dma = pltpu.SemaphoreType.DMA
        return pl.pallas_call(
            functools.partial(kernel, nb, ng),
            out_shape=jax.ShapeDtypeStruct((3, depth, rows, ny), f32),
            in_specs=[
                pl.BlockSpec(memory_space=pltpu.HBM),
                pl.BlockSpec(memory_space=pltpu.HBM),
            ],
            out_specs=pl.BlockSpec(memory_space=pltpu.VMEM),
            scratch_shapes=[
                pltpu.SMEM((bands,), f32),
                pltpu.VMEM((bands, 2, depth, nx, ny), bf16),
                pltpu.VMEM((nb, bands, 2, depth, half, ny), bf16),
                pltpu.VMEM((nb, bands - bands // 2 + 1, 2, depth, half, ny), bf16),
                pltpu.VMEM((nb, bands // 2, 2, depth, half, ny), bf16),
                pltpu.VMEM((nx, nx), bf16),
                pltpu.VMEM((ny, ny), bf16),
                pltpu.VMEM((2, depth, nx, ny), f32),
                pltpu.VMEM((nb - 1, 2, depth, rows, ny), f32),
                pltpu.VMEM((nb, 4, depth, half, ny), f32),
                pltpu.VMEM((4, nb - 1, depth, half, ny), f32),
                pltpu.VMEM((4 * nb, depth, half, ny), f32),
                pltpu.VMEM((2 * nb * bands + 8 * nb - 5 + max(MIXED), depth, half, ny), f32),
                dma,
                dma,
                dma((2, nb)),
                dma((nb,)),
                dma((nb,)),
                dma,
                dma((3,)),
                dma,
                pltpu.SemaphoreType.REGULAR,
                pltpu.SemaphoreType.REGULAR,
            ],
            compiler_params=pltpu.CompilerParams(collective_id=0, has_side_effects=True, vmem_limit_bytes=55000 * 1024),
            name="current",
        )(pltpu.with_memory_space_constraint(occupations, pltpu.HBM), orbitals)

    return jax.shard_map(
        per_device,
        mesh=mesh,
        in_specs=(P("band", None, "grid", None, None), P("band")),
        out_specs=P(None, "grid", "band", None),
        check_vma=False,
    )
```
